32 devices in a mesh: row: 8 (over z, y), col: 4 (over x, core).
Axes of the slice: x: 2, y: 2, z: 4, core: 2. Of those that a mesh axis runs over, the one named last changes fastest.
Arguments:
- image_in: bfloat16 [2048, 1536], P('row', 'col'), may hold values from -6 to 6
- text_in: bfloat16 [2464, 1536], P('row', 'col'), may hold values from -6 to 6
- condition: bfloat16 [16, 1536], P(None, 'row'), may hold values from -6 to 6
- ranges: int32 [16, 2], P('row'), may hold values from 0 to 192, as said below
- mod_weight: bfloat16 [1, 1536, 2, 6, 1536], P(None, 'row', None, None, 'col'), may hold values from -0.15625 to 0.15625
- qkv_weight: bfloat16 [1, 1536, 2, 3, 1536], P(None, 'row', None, None, 'col'), may hold values from -0.15625 to 0.15625
- out_weight: bfloat16 [1, 1536, 2, 1536], P(None, 'row', None, 'col'), may hold values from -2.5 to 2.5
- up_weight: bfloat16 [1, 1536, 2, 6144], P(None, 'row', None, 'col'), may hold values from -0.15625 to 0.15625
- down_weight: bfloat16 [1, 1536, 2, 6144], P(None, 'row', None, 'col'), may hold values from -0.078125 to 0.078125
- image_cot: bfloat16 [2048, 1536], P('row', 'col'), may hold values from -6 to 6
- text_cot: bfloat16 [2464, 1536], P('row', 'col'), may hold values from -6 to 6
Outputs:
- image_out: float32 [2048, 1536], P('row', 'col')
- text_out: float32 [2464, 1536], P('row', 'col')
- grad_image: float32 [2048, 1536], P('row', 'col')
- grad_text: float32 [2464, 1536], P('row', 'col')
- grad_cond: float32 [16, 1536], P(None, 'row')
- grad_mod: float32 [1, 1536, 2, 6, 1536], P(None, 'row', None, None, 'col')
- grad_qkv: float32 [1, 1536, 2, 3, 1536], P(None, 'row', None, None, 'col')
- grad_out: float32 [1, 1536, 2, 1536], P(None, 'row', None, 'col')
- grad_up: float32 [1, 1536, 2, 6144], P(None, 'row', None, 'col')
- grad_down: float32 [1, 1536, 2, 6144], P(None, 'row', None, 'col')
The draws below stay inside these ranges and needn't reach their ends.
Inputs may be any that keep to these rules, and one draw needn't show every extreme that they name: `ranges`: each index of row has 2 slots; the first always holds 154 text rows and a multiple of 64 image rows; the second is empty or holds 154 text rows and exactly the image rows the first leaves over, so that index's 256 image rows are full.
All inputs are finite; a program needn't handle non-finite values.
Results may differ from the reference program's by a relative error of at most 0.015.
The reference program's roundings to bfloat16 on the way count: a program that leaves them out, or rounds other values in their place, can miss the bound.
Values may be sent and summed in bfloat16 or wider, within the bound.
A program may use at most 320 MiB of HBM per device.

```python
import math
import jax
import jax.numpy as jnp
from jax import lax

D = 1536
HEADS = 24
FF = 6144
TXT_LEN = 154
SLOTS = 2
LAYERS = 1
IMG_DEV = 256
HD = 64
TXT_DEV = 308
SEQS = 16
IMG_TOTAL = 2048
TXT_TOTAL = 2464
N_ROW = 8


def draw_ranges(key, part):
    groups = SEQS // SLOTS
    key_length, key_present, key_pick = jax.random.split(key, 3)
    longest = IMG_DEV // 64 - 1
    first = jax.random.randint(key_length, (groups,), 1, longest + 1)
    chosen = jax.random.randint(key_pick, (), 0, groups)
    places = jnp.arange(groups)
    first = jnp.where(places == chosen, longest, first)
    present = (jax.random.randint(key_present, (groups,), 0, 4) > 0).astype(jnp.int32)
    present = jnp.where(places == chosen, 1, present)
    image_first = 64 * first
    image_second = present * (IMG_DEV - image_first)
    text_first = jnp.full((groups,), TXT_LEN, jnp.int32)
    text_second = present * TXT_LEN
    image = jnp.stack([image_first, image_second], axis=1).reshape(-1)
    text = jnp.stack([text_first, text_second], axis=1).reshape(-1)
    return jnp.stack([image, text], axis=1).astype(jnp.int32)


def block_scale(rng, extent, pieces, smallest, high):
    level, own = 1.0, jax.random.fold_in(rng, 6)
    for position, blocks in pieces:
        draws = jnp.exp(jax.random.uniform(jax.random.fold_in(own, position), (blocks,), jnp.float32, smallest / len(pieces), high / len(pieces)))
        level = level * jnp.repeat(draws, extent[position] // blocks).reshape([-1 if axis == position else 1 for axis in range(len(extent))])
    return level


def bell_draw(key, dims, deviation, most, cuts=(), kind=jnp.bfloat16):
    array = jax.random.normal(key, dims, jnp.float32) * deviation
    if len(cuts) > 0:
        array = block_scale(key, dims, cuts, -0.22, 0.18) * array
    return jnp.clip(array, min=-most, max=most).astype(kind)


def setup_inputs(seed: int = 0) -> dict:
    streams_of = jax.random.split(jax.random.key(seed), 12)
    return {
        "image_in": bell_draw(streams_of[0], (IMG_TOTAL, D), 1.0, 6.0, ((0, 8), (1, 4))),
        "text_in": bell_draw(streams_of[1], (TXT_TOTAL, D), 1.0, 6.0, ((0, 8), (1, 4))),
        "condition": bell_draw(streams_of[2], (SEQS, D), 1.0, 6.0, ((1, 8),)),
        "ranges": draw_ranges(jax.random.fold_in(streams_of[11], 71), 0),
        "mod_weight": bell_draw(streams_of[4], (LAYERS, D, 2, 6, D), D ** -0.5, 0.15625, ((1, 8), (4, 4))),
        "qkv_weight": bell_draw(streams_of[5], (LAYERS, D, 2, 3, D), D ** -0.5, 0.15625, ((1, 8), (4, 4))),
        "out_weight": bell_draw(streams_of[6], (LAYERS, D, 2, D), (max(D // 256, 1)) ** -0.5, 2.5, ((1, 8), (3, 4))),
        "up_weight": bell_draw(streams_of[7], (LAYERS, D, 2, FF), D ** -0.5, 0.15625, ((1, 8), (3, 4))),
        "down_weight": bell_draw(streams_of[8], (LAYERS, D, 2, FF), FF ** -0.5, 0.078125, ((1, 8), (3, 4))),
        "image_cot": bell_draw(streams_of[9], (IMG_TOTAL, D), 1.0, 6.0, ((0, 8), (1, 4))),
        "text_cot": bell_draw(streams_of[10], (TXT_TOTAL, D), 1.0, 6.0, ((0, 8), (1, 4))),
    }


EPSILON = 1e-06
HIGHEST = lax.Precision.HIGHEST

def slot_table(lengths, image_rows, text_rows):
    ends = jnp.cumsum(lengths, axis=0, dtype=jnp.int32)
    starts = ends - lengths
    slot_ids = jnp.arange(lengths.shape[0], dtype=jnp.int32)
    tables = []
    segments = []
    for column, amount in ((0, image_rows), (1, text_rows)):
        places = jnp.arange(amount, dtype=jnp.int32)[:, None]
        inside = ((places >= starts[None, :, column]) & (places < ends[None, :, column])).astype(jnp.int32)
        tables.append(inside.astype(jnp.float32))
        filled = lax.optimization_barrier(jnp.sum(inside, axis=1, dtype=jnp.int32))
        segments.append(lax.optimization_barrier(jnp.sum(inside * slot_ids[None, :], axis=1, dtype=jnp.int32)) + lengths.shape[0] * (1 - filled))
    return (jnp.concatenate(tables, axis=0), jnp.concatenate(segments, axis=0))

def group_dot(left, right_image, right_text):
    groups = left.shape[0]
    width = left.shape[2]
    upper = jnp.dot(left[:, :IMG_DEV].reshape(-1, width), right_image, preferred_element_type=jnp.float32)
    lower = jnp.dot(left[:, IMG_DEV:].reshape(-1, width), right_text, preferred_element_type=jnp.float32)
    return jnp.concatenate([upper.reshape(groups, IMG_DEV, -1), lower.reshape(groups, TXT_DEV, -1)], axis=1)

def plain_partial(left, right):
    return jnp.dot(left.T, right, preferred_element_type=jnp.float32)

def group_outer(left, right):
    width = left.shape[2]
    other = right.shape[2]

    def add_group(totals, operands):
        left_rows, right_rows = operands
        upper = totals[0] + plain_partial(left_rows[:IMG_DEV], right_rows[:IMG_DEV])
        lower = totals[1] + plain_partial(left_rows[IMG_DEV:], right_rows[IMG_DEV:])
        return ((upper, lower), None)
    start = (jnp.zeros((width, other), jnp.float32), jnp.zeros((width, other), jnp.float32))
    totals, _ = lax.scan(add_group, start, (left, right))
    return jnp.stack([totals[0], totals[1]], axis=1)

def group_mod(slot_ones, mod_groups, layer_index, component):
    upper = jnp.einsum('gps,gsf->gpf', slot_ones[:, :IMG_DEV], mod_groups[:, :, layer_index, 0, component], precision=HIGHEST)
    lower = jnp.einsum('gps,gsf->gpf', slot_ones[:, IMG_DEV:], mod_groups[:, :, layer_index, 1, component], precision=HIGHEST)
    return jnp.concatenate([upper, lower], axis=1)

def group_slots(slot_ones, rows):
    upper = jnp.einsum('gps,gpf->gsf', slot_ones[:, :IMG_DEV], rows[:, :IMG_DEV], precision=HIGHEST)
    lower = jnp.einsum('gps,gpf->gsf', slot_ones[:, IMG_DEV:], rows[:, IMG_DEV:], precision=HIGHEST)
    return jnp.stack([upper, lower], axis=2)

def normalize(hidden):
    center = lax.optimization_barrier(jnp.mean(hidden, axis=-1, keepdims=True))
    spread = lax.optimization_barrier(jnp.mean(hidden * hidden, axis=-1, keepdims=True)) - center * center
    scaling = lax.rsqrt(spread + EPSILON)
    return ((hidden - center) * scaling, scaling)

def norm_back(grad_hat, normed, scaling):
    first = lax.optimization_barrier(jnp.mean(grad_hat, axis=-1, keepdims=True))
    second = lax.optimization_barrier(jnp.mean(grad_hat * normed, axis=-1, keepdims=True))
    return scaling * (grad_hat - first - normed * second)

def gelu_slope(value):
    coeff = math.sqrt(2.0 / math.pi)
    tangent = jnp.tanh(coeff * (value + 0.044715 * value * value * value))
    return 0.5 * (1.0 + tangent) + 0.5 * value * (1.0 - tangent * tangent) * coeff * (1.0 + 3.0 * 0.044715 * value * value)

def silu_slope(value):
    sigma = jax.nn.sigmoid(value)
    return sigma * (1.0 + value * (1.0 - sigma))

def attend_group(operands, scale):
    queries, key_rows, value_rows, segments = operands
    scores = jnp.einsum('qhd,khd->hqk', queries.astype(jnp.float32), key_rows.astype(jnp.float32)) * scale
    allowed = segments[:, None] == segments[None, :]
    scores = jnp.where(allowed[None], scores, -jnp.inf)
    highest = lax.optimization_barrier(jnp.max(scores, axis=2, keepdims=True))
    log_total = highest + jnp.log(lax.optimization_barrier(jnp.sum(jnp.exp(scores - highest), axis=2, keepdims=True)))
    weights = jnp.exp(scores - log_total).astype(jnp.bfloat16)
    output = jnp.einsum('hqk,khd->qhd', weights.astype(jnp.float32), value_rows.astype(jnp.float32)).astype(jnp.bfloat16)
    return (output, log_total[:, :, 0])

def attend_back_group(operands, scale):
    queries, key_rows, value_rows, output, grad_output, log_total, segments = operands
    scores = jnp.einsum('qhd,khd->hqk', queries.astype(jnp.float32), key_rows.astype(jnp.float32)) * scale
    allowed = segments[:, None] == segments[None, :]
    scores = jnp.where(allowed[None], scores, -jnp.inf)
    probs = jnp.exp(scores - log_total[:, :, None])
    grad_values = jnp.einsum('hqk,qhd->khd', probs.astype(jnp.bfloat16).astype(jnp.float32), grad_output.astype(jnp.float32))
    grad_probs = jnp.einsum('qhd,khd->hqk', grad_output.astype(jnp.float32), value_rows.astype(jnp.float32))
    inner = lax.optimization_barrier(jnp.sum(grad_output.astype(jnp.float32) * output.astype(jnp.float32), axis=2)).T
    grad_scores = (probs * (grad_probs - inner[:, :, None]) * scale).astype(jnp.bfloat16)
    grad_queries = jnp.einsum('hqk,khd->qhd', grad_scores.astype(jnp.float32), key_rows.astype(jnp.float32))
    grad_keys = jnp.einsum('hqk,qhd->khd', grad_scores.astype(jnp.float32), queries.astype(jnp.float32))
    return jnp.stack([grad_queries, grad_keys, grad_values], axis=1).astype(jnp.bfloat16)

def reference(image_in, text_in, condition, ranges, mod_weight, qkv_weight, out_weight, up_weight, down_weight, image_cot, text_cot):
    groups = N_ROW
    rows_all = IMG_DEV + TXT_DEV
    scale = 1.0 / math.sqrt(HD)
    slot_ones, segments = jax.vmap(lambda table: slot_table(table, IMG_DEV, TXT_DEV))(ranges.reshape(groups, SLOTS, 2))
    silu_cond = jax.nn.silu(condition.astype(jnp.float32)).astype(jnp.bfloat16)
    mod_all = jnp.einsum('sd,ldxkf->slxkf', silu_cond.astype(jnp.float32), mod_weight.astype(jnp.float32))
    mod_groups = mod_all.reshape(groups, SLOTS, LAYERS, 2, 6, D)
    hidden = jnp.concatenate([image_in.reshape(groups, IMG_DEV, D), text_in.reshape(groups, TXT_DEV, D)], axis=1).astype(jnp.float32)
    saved = []
    for layer_index in range(LAYERS):
        mods = [group_mod(slot_ones, mod_groups, layer_index, part_no) for part_no in range(6)]
        qkv_flat = qkv_weight[layer_index].reshape(D, 2, 3 * D)
        normed_one, scaling_one = normalize(hidden)
        modulated_one = (normed_one * (1.0 + mods[1]) + mods[0]).astype(jnp.bfloat16)
        projected = group_dot(modulated_one, qkv_flat[:, 0], qkv_flat[:, 1]).astype(jnp.bfloat16)
        heads_form = projected.reshape(groups, rows_all, 3, HEADS, HD)
        attended, log_totals = lax.map(lambda operands: attend_group(operands, scale), (heads_form[:, :, 0], heads_form[:, :, 1], heads_form[:, :, 2], segments))
        mixed = attended.reshape(groups, rows_all, D)
        branch_one = group_dot(mixed, out_weight[layer_index][:, 0].T, out_weight[layer_index][:, 1].T)
        midway = hidden + mods[2] * branch_one
        normed_two, scaling_two = normalize(midway)
        modulated_two = (normed_two * (1.0 + mods[4]) + mods[3]).astype(jnp.bfloat16)
        lifted = group_dot(modulated_two, up_weight[layer_index][:, 0], up_weight[layer_index][:, 1])
        activated = jax.nn.gelu(lifted, approximate=True).astype(jnp.bfloat16)
        branch_two = group_dot(activated, down_weight[layer_index][:, 0].T, down_weight[layer_index][:, 1].T)
        hidden = midway + mods[5] * branch_two
        saved.append((normed_one, scaling_one, modulated_one, heads_form, attended, log_totals, branch_one, normed_two, scaling_two, modulated_two, lifted, activated, branch_two))
    image_out = hidden[:, :IMG_DEV].reshape(-1, D)
    text_out = hidden[:, IMG_DEV:].reshape(-1, D)
    grad_hidden = jnp.concatenate([image_cot.reshape(groups, IMG_DEV, D), text_cot.reshape(groups, TXT_DEV, D)], axis=1).astype(jnp.float32)
    grads_qkv = [None] * LAYERS
    grads_out = [None] * LAYERS
    grads_up = [None] * LAYERS
    grads_down = [None] * LAYERS
    grads_slots = [None] * LAYERS
    for layer_index in reversed(range(LAYERS)):
        normed_one, scaling_one, modulated_one, heads_form, attended, log_totals, branch_one, normed_two, scaling_two, modulated_two, lifted, activated, branch_two = saved[layer_index]
        mods = [group_mod(slot_ones, mod_groups, layer_index, part_no) for part_no in range(6)]
        qkv_flat = qkv_weight[layer_index].reshape(D, 2, 3 * D)
        grad_branch_two = (grad_hidden * mods[5]).astype(jnp.bfloat16)
        gate_two_rows = grad_hidden * branch_two
        grad_act = group_dot(grad_branch_two, down_weight[layer_index][:, 0], down_weight[layer_index][:, 1])
        grad_lifted = (grad_act * gelu_slope(lifted)).astype(jnp.bfloat16)
        grads_down[layer_index] = group_outer(grad_branch_two, activated)
        grads_up[layer_index] = group_outer(modulated_two, grad_lifted)
        grad_mod_two = group_dot(grad_lifted, up_weight[layer_index][:, 0].T, up_weight[layer_index][:, 1].T)
        shift_two_rows = grad_mod_two
        scale_two_rows = grad_mod_two * normed_two
        grad_hidden = grad_hidden + norm_back(grad_mod_two * (1.0 + mods[4]), normed_two, scaling_two)
        grad_branch_one = (grad_hidden * mods[2]).astype(jnp.bfloat16)
        gate_one_rows = grad_hidden * branch_one
        grad_mixed = group_dot(grad_branch_one, out_weight[layer_index][:, 0], out_weight[layer_index][:, 1]).astype(jnp.bfloat16)
        grads_out[layer_index] = group_outer(grad_branch_one, attended.reshape(groups, rows_all, D))
        grad_heads = grad_mixed.reshape(groups, rows_all, HEADS, HD)
        grad_parts = lax.map(lambda operands: attend_back_group(operands, scale), (heads_form[:, :, 0], heads_form[:, :, 1], heads_form[:, :, 2], attended, grad_heads, log_totals, segments))
        grad_projected = grad_parts.reshape(groups, rows_all, 3 * D)
        grads_qkv[layer_index] = group_outer(modulated_one, grad_projected).reshape(D, 2, 3, D)
        grad_mod_one = group_dot(grad_projected, qkv_flat[:, 0].T, qkv_flat[:, 1].T)
        shift_one_rows = grad_mod_one
        scale_one_rows = grad_mod_one * normed_one
        grad_hidden = grad_hidden + norm_back(grad_mod_one * (1.0 + mods[1]), normed_one, scaling_one)
        rows_list = [shift_one_rows, scale_one_rows, gate_one_rows, shift_two_rows, scale_two_rows, gate_two_rows]
        grads_slots[layer_index] = jnp.stack([group_slots(slot_ones, rows) for rows in rows_list], axis=3)
    mod_grads = jnp.stack(grads_slots, axis=2).reshape(SEQS, LAYERS, 2, 6, D)
    grad_mod = jnp.einsum('sd,slxkf->ldxkf', silu_cond.astype(jnp.float32), mod_grads, precision=HIGHEST)
    grad_cond = jnp.einsum('slxkf,ldxkf->sd', mod_grads, mod_weight.astype(jnp.float32), precision=HIGHEST) * silu_slope(condition.astype(jnp.float32))
    grad_image = grad_hidden[:, :IMG_DEV].reshape(-1, D)
    grad_text = grad_hidden[:, IMG_DEV:].reshape(-1, D)
    return (image_out, text_out, grad_image, grad_text, grad_cond, grad_mod, jnp.stack(grads_qkv), jnp.stack(grads_out), jnp.stack(grads_up), jnp.stack(grads_down))
```

```python
import math

import jax
import jax.numpy as jnp
from jax import lax
from jax.sharding import PartitionSpec as P

D = 1536
LAYERS = 1
IMG_DEV = 256
HD = 64
TXT_DEV = 308


EPSILON = 1e-06
HIGHEST = lax.Precision.HIGHEST


BF16 = jnp.bfloat16
F32 = jnp.float32
RING_LIMIT = 8


class Ring:
    def __init__(self, count):
        order = list(range(0, count, 2)) + list(range(count - 1, 0, -2))
        forward = [(order[k], order[(k + 1) % count]) for k in range(count)]
        self.count = count
        self.perms = (forward, [(target, source) for source, target in forward])
        self.order = jnp.array(order, jnp.int32)
        places = jnp.array([order.index(index) for index in range(count)], jnp.int32)
        self.place = places[lax.axis_index("row")]

    def owner(self, way, step):
        shift = -step if way == 0 else step
        return self.order[(self.place + shift + self.count) % self.count]


def after(value, gate):
    if gate is None:
        return value
    return lax.optimization_barrier((value, gate))[0]


def spans_of(width):
    half = width // 256 * 128
    return ((0, half), (half, width))


def gather_weight(ring, weight, gates):
    rows, _, width = weight.shape
    if ring is None:
        whole = lax.all_gather(weight, "row", axis=0, tiled=True)
        return (whole[:, 0], whole[:, 1]), (None, None)
    wholes, late = [], []
    for way in range(2):
        whole = jnp.zeros((ring.count, rows, width), weight.dtype)
        whole = lax.dynamic_update_slice(whole, weight[None, :, way], (ring.owner(way, 0), 0, 0))
        pieces = [after(weight[:, way, low:high], gates[way]) for low, high in spans_of(width)]
        for step in range(1, ring.count):
            if step == ring.count - 1:
                late.append(pieces[0])
            for number, (low, _) in enumerate(spans_of(width)):
                pieces[number] = lax.ppermute(pieces[number], "row", ring.perms[way])
                whole = lax.dynamic_update_slice(
                    whole, pieces[number][None], (ring.owner(way, step), 0, low)
                )
        wholes.append(whole.reshape(-1, width))
    return tuple(wholes), tuple(late)


def scatter_grads(ring, parts):
    width = parts[0].shape[1]
    if ring is None:
        return jnp.stack(
            [lax.psum_scatter(part.astype(BF16), "row", scatter_dimension=0, tiled=True) for part in parts],
            axis=1,
        ).astype(F32)
    streams = []
    for way, part in enumerate(parts):
        blocks = part.reshape(ring.count, -1, width)
        pieces = []
        for low, high in spans_of(width):
            total = None
            for step in range(ring.count):
                own = lax.dynamic_index_in_dim(blocks, ring.owner(way, step + 1), 0, False)[:, low:high]
                if total is None:
                    total = own
                else:
                    total = lax.ppermute(total.astype(BF16), "row", ring.perms[way]).astype(F32) + own
            pieces.append(total)
        streams.append(jnp.concatenate(pieces, axis=1))
    return jnp.stack(streams, axis=1)


def rotations(count):
    return [[(index, (index + turn) % count) for index in range(count)] for turn in range(1, count)]


def exchange_sum(ring, values):
    if ring is None:
        return lax.psum_scatter(values, "row", scatter_dimension=0, tiled=True)
    blocks = values.reshape((ring.count, -1) + values.shape[1:])
    me = lax.axis_index("row")
    total = lax.dynamic_index_in_dim(blocks, me, 0, False)
    for turn, perm in enumerate(rotations(ring.count), 1):
        block = lax.dynamic_index_in_dim(blocks, (me + turn) % ring.count, 0, False)
        total = total + lax.ppermute(block, "row", perm)
    return total


def spread_all(ring, values):
    if ring is None:
        return lax.all_gather(values, "row", axis=0, tiled=True)
    me = lax.axis_index("row")
    start = (0,) * values.ndim
    whole = jnp.zeros((ring.count,) + values.shape, values.dtype)
    whole = lax.dynamic_update_slice(whole, values[None], (me,) + start)
    for turn, perm in enumerate(rotations(ring.count), 1):
        source = (me - turn + ring.count) % ring.count
        whole = lax.dynamic_update_slice(whole, lax.ppermute(values, "row", perm)[None], (source,) + start)
    return whole.reshape((-1,) + values.shape[1:])


def slot_table(lengths, image_rows, text_rows):
    ends = jnp.cumsum(lengths, axis=0, dtype=jnp.int32)
    starts = ends - lengths
    slot_ids = jnp.arange(lengths.shape[0], dtype=jnp.int32)
    tables = []
    segments = []
    for column, amount in ((0, image_rows), (1, text_rows)):
        places = jnp.arange(amount, dtype=jnp.int32)[:, None]
        inside = ((places >= starts[None, :, column]) & (places < ends[None, :, column])).astype(
            jnp.int32
        )
        tables.append(inside.astype(jnp.float32))
        filled = jnp.sum(inside, axis=1, dtype=jnp.int32)
        segments.append(
            jnp.sum(inside * slot_ids[None, :], axis=1, dtype=jnp.int32)
            + lengths.shape[0] * (1 - filled)
        )
    return (jnp.concatenate(tables, axis=0), jnp.concatenate(segments, axis=0))


def stream_dot(left, right_image, right_text):
    upper = jnp.dot(left[:IMG_DEV], right_image, preferred_element_type=jnp.float32)
    lower = jnp.dot(left[IMG_DEV:], right_text, preferred_element_type=jnp.float32)
    return jnp.concatenate([upper, lower], axis=0)


def stream_outer(left, right):
    upper = jnp.einsum(
        "nk,nf->kf", left[:IMG_DEV], right[:IMG_DEV], preferred_element_type=jnp.float32
    )
    lower = jnp.einsum(
        "nk,nf->kf", left[IMG_DEV:], right[IMG_DEV:], preferred_element_type=jnp.float32
    )
    return (upper, lower)


def row_mod(slot_ones, mod_mine, layer_index, component):
    upper = jnp.dot(slot_ones[:IMG_DEV], mod_mine[:, layer_index, 0, component], precision=HIGHEST)
    lower = jnp.dot(slot_ones[IMG_DEV:], mod_mine[:, layer_index, 1, component], precision=HIGHEST)
    return jnp.concatenate([upper, lower], axis=0)


def slot_sums(slot_ones, rows):
    upper = jnp.dot(slot_ones[:IMG_DEV].T, rows[:IMG_DEV], precision=HIGHEST)
    lower = jnp.dot(slot_ones[IMG_DEV:].T, rows[IMG_DEV:], precision=HIGHEST)
    return jnp.stack([upper, lower], axis=1)


def feature_sums(first, second):
    return lax.psum((jnp.sum(first, axis=1), jnp.sum(second, axis=1)), "col")


def normalize(hidden):
    totals, squares = feature_sums(hidden, hidden * hidden)
    center = totals / D
    spread = squares / D - center * center
    scaling = lax.rsqrt(spread + EPSILON)
    return ((hidden - center[:, None]) * scaling[:, None], scaling[:, None])


def norm_back(grad_hat, normed, scaling):
    first, second = feature_sums(grad_hat, grad_hat * normed)
    return scaling * (grad_hat - first[:, None] / D - normed * (second[:, None] / D))


def gelu_slope(value):
    coeff = math.sqrt(2.0 / math.pi)
    tangent = jnp.tanh(coeff * (value + 0.044715 * value * value * value))
    return 0.5 * (1.0 + tangent) + 0.5 * value * (1.0 - tangent * tangent) * coeff * (
        1.0 + 3.0 * 0.044715 * value * value
    )


def silu_slope(value):
    sigma = jax.nn.sigmoid(value)
    return sigma * (1.0 + value * (1.0 - sigma))


def gather_features(values):
    return lax.all_gather(values, "col", axis=1, tiled=True)


def gather_grads(values):
    return lax.all_gather(values, "col", axis=1, tiled=True)


def scatter_features(values):
    return lax.psum_scatter(values, "col", scatter_dimension=1, tiled=True)


def scatter_back(values):
    return lax.psum_scatter(values, "col", scatter_dimension=1, tiled=True)


def stream_dot_back(left, right_image, right_text):
    return stream_dot(left, right_image.T, right_text.T)


def attend_head(operands, segments, scale):
    queries, key_rows, value_rows = operands
    scores = jnp.dot(queries, key_rows.T, preferred_element_type=jnp.float32) * scale
    allowed = segments[:, None] == segments[None, :]
    scores = jnp.where(allowed, scores, -jnp.inf)
    highest = jnp.max(scores, axis=1, keepdims=True)
    log_total = highest + jnp.log(jnp.sum(jnp.exp(scores - highest), axis=1, keepdims=True))
    weights = jnp.exp(scores - log_total).astype(jnp.bfloat16)
    output = jnp.dot(weights, value_rows, preferred_element_type=jnp.float32).astype(jnp.bfloat16)
    return (output, log_total[:, 0])


def attend_back_head(operands, segments, scale):
    queries, key_rows, value_rows, output, grad_output, log_total = operands
    scores = jnp.dot(queries, key_rows.T, preferred_element_type=jnp.float32) * scale
    allowed = segments[:, None] == segments[None, :]
    scores = jnp.where(allowed, scores, -jnp.inf)
    probs = jnp.exp(scores - log_total[:, None])
    grad_values = jnp.dot(
        probs.astype(jnp.bfloat16).T, grad_output, preferred_element_type=jnp.float32
    )
    grad_probs = jnp.dot(grad_output, value_rows.T, preferred_element_type=jnp.float32)
    inner = jnp.sum(
        grad_output.astype(jnp.float32) * output.astype(jnp.float32), axis=1, keepdims=True
    )
    grad_scores = (probs * (grad_probs - inner) * scale).astype(jnp.bfloat16)
    grad_queries = jnp.dot(grad_scores, key_rows, preferred_element_type=jnp.float32)
    grad_keys = jnp.dot(grad_scores.T, queries, preferred_element_type=jnp.float32)
    return jnp.stack([grad_queries, grad_keys, grad_values], axis=0).astype(jnp.bfloat16)


def per_device(
    image_in,
    text_in,
    condition,
    ranges,
    mod_weight,
    qkv_weight,
    out_weight,
    up_weight,
    down_weight,
    image_cot,
    text_cot,
):
    slot_ones, segments = slot_table(ranges, IMG_DEV, TXT_DEV)
    col_width = image_in.shape[1]
    row_count = qkv_weight.shape[1]
    heads_here = col_width // HD
    scale = 1.0 / math.sqrt(HD)
    silu_cond = jax.nn.silu(condition.astype(jnp.float32)).astype(jnp.bfloat16)
    size = lax.axis_size("row")
    ring = Ring(size) if size <= RING_LIMIT else None
    mod_terms = jnp.einsum(
        "sd,ldxkf->slxkf", silu_cond, mod_weight, preferred_element_type=jnp.float32
    )
    mod_mine = exchange_sum(ring, mod_terms)
    qkv_whole, late = gather_weight(
        ring, qkv_weight[0].reshape(row_count, 2, 3 * col_width), (None, None)
    )
    out_whole, _ = gather_weight(ring, out_weight[0], (None, None))
    up_whole, late = gather_weight(ring, up_weight[0], late)
    down_whole, _ = gather_weight(ring, down_weight[0], late)
    hidden = jnp.concatenate([image_in, text_in], axis=0).astype(jnp.float32)
    layer_index = 0
    mods = [row_mod(slot_ones, mod_mine, layer_index, part_no) for part_no in range(6)]
    normed_one, scaling_one = normalize(hidden)
    modulated_one = (normed_one * (1.0 + mods[1]) + mods[0]).astype(jnp.bfloat16)
    gathered_one = gather_features(modulated_one)
    projected = stream_dot(gathered_one, *qkv_whole).astype(jnp.bfloat16)
    heads_form = projected.reshape(-1, 3, heads_here, HD).transpose(1, 2, 0, 3)
    attended, log_totals = lax.map(
        lambda operands: attend_head(operands, segments, scale),
        (heads_form[0], heads_form[1], heads_form[2]),
    )
    mixed = attended.transpose(1, 0, 2).reshape(-1, col_width)
    branch_one = scatter_features(stream_dot_back(mixed, *out_whole))
    midway = hidden + mods[2] * branch_one
    normed_two, scaling_two = normalize(midway)
    modulated_two = (normed_two * (1.0 + mods[4]) + mods[3]).astype(jnp.bfloat16)
    gathered_two = gather_features(modulated_two)
    lifted = stream_dot(gathered_two, *up_whole)
    activated = jax.nn.gelu(lifted, approximate=True).astype(jnp.bfloat16)
    branch_two = scatter_features(stream_dot_back(activated, *down_whole))
    hidden = midway + mods[5] * branch_two
    saved = [
        (
            normed_one,
            scaling_one,
            gathered_one,
            heads_form,
            attended,
            log_totals,
            mixed,
            branch_one,
            normed_two,
            scaling_two,
            gathered_two,
            lifted,
            activated,
            branch_two,
        )
    ]
    image_out = hidden[:IMG_DEV]
    text_out = hidden[IMG_DEV:]
    grad_hidden = jnp.concatenate([image_cot, text_cot], axis=0).astype(jnp.float32)
    grads_qkv = [None] * LAYERS
    grads_out = [None] * LAYERS
    grads_up = [None] * LAYERS
    grads_down = [None] * LAYERS
    grads_slots = [None] * LAYERS
    for layer_index in reversed(range(LAYERS)):
        (
            normed_one,
            scaling_one,
            gathered_one,
            heads_form,
            attended,
            log_totals,
            mixed,
            branch_one,
            normed_two,
            scaling_two,
            gathered_two,
            lifted,
            activated,
            branch_two,
        ) = saved[layer_index]
        mods = [row_mod(slot_ones, mod_mine, layer_index, part_no) for part_no in range(6)]
        grad_branch_two = (grad_hidden * mods[5]).astype(jnp.bfloat16)
        gate_two_rows = grad_hidden * branch_two
        grad_full_two = gather_grads(grad_branch_two)
        grad_act = stream_dot(grad_full_two, *down_whole)
        grad_lifted = (grad_act * gelu_slope(lifted)).astype(jnp.bfloat16)
        grads_down[layer_index] = scatter_grads(ring, stream_outer(grad_full_two, activated))
        grads_up[layer_index] = scatter_grads(ring, stream_outer(gathered_two, grad_lifted))
        grad_mod_two = scatter_back(stream_dot_back(grad_lifted, *up_whole))
        scale_two_rows = grad_mod_two * normed_two
        grad_hidden = grad_hidden + norm_back(
            grad_mod_two * (1.0 + mods[4]), normed_two, scaling_two
        )
        grad_branch_one = (grad_hidden * mods[2]).astype(jnp.bfloat16)
        gate_one_rows = grad_hidden * branch_one
        grad_full_one = gather_grads(grad_branch_one)
        grad_mixed = stream_dot(grad_full_one, *out_whole).astype(jnp.bfloat16)
        grad_heads = grad_mixed.reshape(-1, heads_here, HD).transpose(1, 0, 2)
        grad_parts = lax.map(
            lambda operands: attend_back_head(operands, segments, scale),
            (heads_form[0], heads_form[1], heads_form[2], attended, grad_heads, log_totals),
        )
        grad_projected = grad_parts.transpose(2, 1, 0, 3).reshape(-1, 3 * col_width)
        grads_out[layer_index] = scatter_grads(ring, stream_outer(grad_full_one, mixed))
        grads_qkv[layer_index] = scatter_grads(
            ring, stream_outer(gathered_one, grad_projected)
        ).reshape(row_count, 2, 3, col_width)
        grad_mod_one = scatter_back(stream_dot_back(grad_projected, *qkv_whole))
        scale_one_rows = grad_mod_one * normed_one
        grad_hidden = grad_hidden + norm_back(
            grad_mod_one * (1.0 + mods[1]), normed_one, scaling_one
        )
        rows_list = [
            grad_mod_one,
            scale_one_rows,
            gate_one_rows,
            grad_mod_two,
            scale_two_rows,
            gate_two_rows,
        ]
        grads_slots[layer_index] = jnp.stack(
            [slot_sums(slot_ones, rows) for rows in rows_list], axis=2
        )
    mod_all = spread_all(ring, jnp.stack(grads_slots, axis=1))
    grad_mod = jnp.einsum(
        "sd,slxkf->ldxkf", silu_cond.astype(jnp.float32), mod_all, precision=HIGHEST
    )
    cond_part = jnp.einsum(
        "slxkf,ldxkf->sd", mod_all, mod_weight.astype(jnp.float32), precision=HIGHEST
    )
    cond_total = lax.psum(cond_part, "col")
    grad_cond = cond_total * silu_slope(condition.astype(jnp.float32))
    grad_image = grad_hidden[:IMG_DEV]
    grad_text = grad_hidden[IMG_DEV:]
    return (
        image_out,
        text_out,
        grad_image,
        grad_text,
        grad_cond,
        grad_mod,
        jnp.stack(grads_qkv),
        jnp.stack(grads_out),
        jnp.stack(grads_up),
        jnp.stack(grads_down),
    )


def solution(mesh):
    return jax.shard_map(
        per_device,
        mesh=mesh,
        in_specs=(
            P("row", "col"),
            P("row", "col"),
            P(None, "row"),
            P("row", None),
            P(None, "row", None, None, "col"),
            P(None, "row", None, None, "col"),
            P(None, "row", None, "col"),
            P(None, "row", None, "col"),
            P(None, "row", None, "col"),
            P("row", "col"),
            P("row", "col"),
        ),
        out_specs=(
            P("row", "col"),
            P("row", "col"),
            P("row", "col"),
            P("row", "col"),
            P(None, "row"),
            P(None, "row", None, None, "col"),
            P(None, "row", None, None, "col"),
            P(None, "row", None, "col"),
            P(None, "row", None, "col"),
            P(None, "row", None, "col"),
        ),
        check_vma=False,
    )
```

```python
import functools
import math

import jax
import jax.numpy as jnp
from jax import lax
from jax.experimental import pallas as pl
from jax.experimental.pallas import tpu as pltpu
from jax.sharding import PartitionSpec as P

D = 1536
IMG_DEV = 256
HD = 64
TXT_DEV = 308
ROWS = IMG_DEV + TXT_DEV

EPSILON = 1e-06
HIGHEST = lax.Precision.HIGHEST
BF16 = jnp.bfloat16
F32 = jnp.float32
RING_LIMIT = 8


class Ring:
    def __init__(self, count):
        order = list(range(0, count, 2)) + list(range(count - 1, 0, -2))
        forward = [(order[k], order[(k + 1) % count]) for k in range(count)]
        self.count = count
        self.perms = (forward, [(target, source) for source, target in forward])
        me = lax.axis_index("row")
        self.me = me
        self.place = jnp.where((me & 1) == 0, me >> 1, count - 1 - (me >> 1))
        self.owners = {}

    def wrap(self, value):
        if self.count & (self.count - 1) == 0:
            return value & (self.count - 1)
        return lax.rem(value + self.count, self.count)

    def owner(self, way, step):
        shift = (-step if way == 0 else step) % self.count
        if shift not in self.owners:
            spot = self.wrap(self.place + shift) if shift else self.place
            self.owners[shift] = jnp.where(
                spot < self.count // 2, spot << 1, 2 * self.count - 1 - (spot << 1)
            )
        return self.owners[shift]


def after(value, gate):
    if gate is None:
        return value
    return lax.optimization_barrier((value, gate))[0]


def gather_pieces(ring, pieces, gates):
    if ring is None:
        wholes = [[lax.all_gather(piece, "row", axis=0, tiled=True) for piece in group] for group in pieces]
        return wholes, None
    wholes, arrivals = [], []
    for way in range(2):
        held = list(pieces[way])
        built = []
        for piece in held:
            rows = piece.shape[0]
            whole = jnp.zeros((rows * ring.count, piece.shape[1]), piece.dtype)
            built.append(lax.dynamic_update_slice(whole, piece, (ring.owner(way, 0) * rows, 0)))
        if gates is not None:
            held = [after(piece, gate) for piece, gate in zip(held, gates[way])]
        seen = []
        for step in range(1, ring.count):
            for number, piece in enumerate(held):
                held[number] = lax.ppermute(piece, "row", ring.perms[way])
                rows = piece.shape[0]
                built[number] = lax.dynamic_update_slice(
                    built[number], held[number], (ring.owner(way, step) * rows, 0)
                )
            seen.append(list(held))
        wholes.append(built)
        arrivals.append(seen)
    return wholes, arrivals


def scatter_pieces(ring, pieces, gates):
    if ring is None:
        count = lax.axis_size("row")
        results = []
        for group in pieces:
            results.append(
                [
                    lax.psum_scatter(
                        jnp.concatenate([part(index) for index in range(count)], axis=0).astype(BF16),
                        "row",
                        scatter_dimension=0,
                        tiled=True,
                    ).astype(F32)
                    for part in group
                ]
            )
        return results, None
    results, arrivals = [], []
    for way in range(2):
        totals = [part(ring.owner(way, 1)).astype(BF16) for part in pieces[way]]
        if gates is not None:
            totals = [after(total, gate) for total, gate in zip(totals, gates[way])]
        seen = []
        for step in range(1, ring.count):
            for number, part in enumerate(pieces[way]):
                came = lax.ppermute(totals[number], "row", ring.perms[way])
                totals[number] = came.astype(F32) + part(ring.owner(way, step + 1))
                if step < ring.count - 1:
                    totals[number] = totals[number].astype(BF16)
                seen.append(came)
            seen[-len(pieces[way]) :] = [seen[-len(pieces[way]) :]]
        results.append(totals)
        arrivals.append(seen)
    return results, arrivals


def rotations(count):
    return [[(index, (index + turn) % count) for index in range(count)] for turn in range(1, count)]


def exchange_sum(ring, values):
    if ring is None:
        return lax.psum_scatter(values, "row", scatter_dimension=0, tiled=True)
    blocks = values.reshape((ring.count, -1) + values.shape[1:])
    total = lax.dynamic_index_in_dim(blocks, ring.me, 0, False)
    for turn, perm in enumerate(rotations(ring.count), 1):
        block = lax.dynamic_index_in_dim(blocks, ring.wrap(ring.me + turn), 0, False)
        total = total + lax.ppermute(block, "row", perm)
    return total


def spread_all(ring, values):
    if ring is None:
        return lax.all_gather(values, "row", axis=0, tiled=True)
    start = (0,) * values.ndim
    whole = jnp.zeros((ring.count,) + values.shape, values.dtype)
    whole = lax.dynamic_update_slice(whole, values[None], (ring.me,) + start)
    for turn, perm in enumerate(rotations(ring.count), 1):
        source = ring.wrap(ring.me + ring.count - turn)
        whole = lax.dynamic_update_slice(whole, lax.ppermute(values, "row", perm)[None], (source,) + start)
    return whole.reshape((-1,) + values.shape[1:])


def swaps(bit):
    return [(index, index ^ bit) for index in range(4)]


def gather_features(values):
    if lax.axis_size("col") != 4:
        return lax.all_gather(values, "col", axis=1, tiled=True)
    me = lax.axis_index("col")
    odd, high = (me & 1) == 1, (me & 2) == 2
    far = lax.ppermute(values, "col", swaps(2))
    near = lax.ppermute(values, "col", swaps(1))
    diagonal = lax.ppermute(far, "col", swaps(1))
    mine = [jnp.where(odd, near, values), jnp.where(odd, values, near)]
    other = [jnp.where(odd, diagonal, far), jnp.where(odd, far, diagonal)]
    return jnp.concatenate(
        [jnp.where(high, other[0], mine[0]), jnp.where(high, other[1], mine[1])]
        + [jnp.where(high, mine[0], other[0]), jnp.where(high, mine[1], other[1])],
        axis=1,
    )


def scatter_features(values):
    if lax.axis_size("col") != 4:
        return lax.psum_scatter(values, "col", scatter_dimension=1, tiled=True)
    me = lax.axis_index("col")
    odd, high = (me & 1) == 1, (me & 2) == 2
    width = values.shape[1] // 4
    blocks = [values[:, index * width : (index + 1) * width] for index in range(4)]
    away = jnp.concatenate([jnp.where(odd, blocks[0], blocks[1]), jnp.where(odd, blocks[2], blocks[3])], axis=1)
    came = lax.ppermute(away, "col", swaps(1))
    low_sum = jnp.where(odd, blocks[1], blocks[0]) + came[:, :width]
    high_sum = jnp.where(odd, blocks[3], blocks[2]) + came[:, width:]
    last = lax.ppermute(jnp.where(high, low_sum, high_sum).astype(BF16), "col", swaps(2))
    return jnp.where(high, high_sum, low_sum) + last.astype(F32)


def slot_table(lengths, image_rows, text_rows):
    slots = lengths.shape[0]
    tables = []
    segments = []
    for column, amount in ((0, image_rows), (1, text_rows)):
        places = jnp.arange(amount, dtype=jnp.int32)[:, None]
        low = jnp.zeros((), jnp.int32)
        segment = jnp.full((amount, 1), slots, jnp.int32)
        for slot in range(slots):
            high = low + lengths[slot, column]
            inside = (places >= low) & (places < high)
            tables.append(inside.astype(F32))
            segment = jnp.where(inside, slot, segment)
            low = high
        segments.append(segment)
    pairs = [jnp.concatenate([tables[slot], tables[slots + slot]], axis=0) for slot in range(slots)]
    return pairs, jnp.concatenate(segments, axis=0)


def stream_dot(left, right_image, right_text):
    upper = jnp.dot(left[:IMG_DEV], right_image, preferred_element_type=F32)
    lower = jnp.dot(left[IMG_DEV:], right_text, preferred_element_type=F32)
    return jnp.concatenate([upper, lower], axis=0)


def stream_dot_back(left, right_image, right_text):
    return stream_dot(left, right_image.T, right_text.T)


def row_mod(members, mod_mine, component):
    streams = []
    for stream, (low, high) in enumerate(((0, IMG_DEV), (IMG_DEV, ROWS))):
        total = None
        for slot, member in enumerate(members):
            term = member[low:high] * mod_mine[slot, 0, stream, component][None, :]
            total = term if total is None else total + term
        streams.append(total)
    return jnp.concatenate(streams, axis=0)


def slot_sums(slot_ones, rows):
    upper = jnp.dot(slot_ones[:IMG_DEV].T, rows[:IMG_DEV], precision=HIGHEST)
    lower = jnp.dot(slot_ones[IMG_DEV:].T, rows[IMG_DEV:], precision=HIGHEST)
    return jnp.stack([upper, lower], axis=1)


def feature_sums(first, second):
    return lax.psum((jnp.sum(first, axis=1), jnp.sum(second, axis=1)), "col")


def normalize(hidden):
    totals, squares = feature_sums(hidden, hidden * hidden)
    center = totals / D
    spread = squares / D - center * center
    scaling = lax.rsqrt(spread + EPSILON)
    return ((hidden - center[:, None]) * scaling[:, None], scaling[:, None])


def norm_back(grad_hat, normed, scaling):
    first, second = feature_sums(grad_hat, grad_hat * normed)
    return scaling * (grad_hat - first[:, None] / D - normed * (second[:, None] / D))


def gelu_slope(value):
    coeff = math.sqrt(2.0 / math.pi)
    tangent = jnp.tanh(coeff * (value + 0.044715 * value * value * value))
    return 0.5 * (1.0 + tangent) + 0.5 * value * (1.0 - tangent * tangent) * coeff * (
        1.0 + 3.0 * 0.044715 * value * value
    )


def silu_slope(value):
    sigma = jax.nn.sigmoid(value)
    return sigma * (1.0 + value * (1.0 - sigma))


def across(left, right):
    return lax.dot_general(left, right, (((1,), (1,)), ((), ())), preferred_element_type=F32)


def down(left, right):
    return lax.dot_general(left, right, (((0,), (0,)), ((), ())), preferred_element_type=F32)


def attend_kernel(q_ref, k_ref, v_ref, seg_keys, seg_queries, out_ref, lse_ref):
    allowed = seg_keys[...] == seg_queries[...]
    for half in range(2):
        lanes = slice(half * HD, (half + 1) * HD)
        queries, key_rows, value_rows = q_ref[:, lanes], k_ref[:, lanes], v_ref[:, lanes]
        scores = jnp.where(allowed, across(key_rows, queries) * (1.0 / math.sqrt(HD)), -jnp.inf)
        highest = jnp.max(scores, axis=0, keepdims=True)
        powers = jnp.exp(scores - highest)
        total = jnp.sum(powers, axis=0, keepdims=True)
        weights = (powers * (1.0 / total)).astype(BF16)
        out_ref[:, lanes] = down(value_rows, weights).T.astype(BF16)
        lse_ref[0, half : half + 1, :] = highest + jnp.log(total)


def attend(queries_keys, value_rows, segments):
    rows, width = value_rows.shape
    pairs = width // (2 * HD)
    block = (rows, 2 * HD)
    return pl.pallas_call(
        attend_kernel,
        grid=(pairs,),
        in_specs=[
            pl.BlockSpec(block, lambda i: (0, i)),
            pl.BlockSpec(block, lambda i: (0, pairs + i)),
            pl.BlockSpec(block, lambda i: (0, i)),
            pl.BlockSpec((rows, 1), lambda i: (0, 0)),
            pl.BlockSpec((1, rows), lambda i: (0, 0)),
        ],
        out_specs=[
            pl.BlockSpec(block, lambda i: (0, i)),
            pl.BlockSpec((1, 8, rows), lambda i: (i, 0, 0)),
        ],
        out_shape=[
            jax.ShapeDtypeStruct((rows, width), BF16),
            jax.ShapeDtypeStruct((pairs, 8, rows), F32),
        ],
        cost_estimate=pl.CostEstimate(
            flops=20 * rows * rows * width, bytes_accessed=10 * rows * width, transcendentals=6 * rows * rows
        ),
        name="attend",
    )(queries_keys, queries_keys, value_rows, segments, segments.reshape(1, rows))


def attend_back_kernel(
    q_ref, k_ref, v_ref, out_ref, grad_ref, lse_ref, seg_keys, seg_queries, dq_ref, dk_ref, dv_ref
):
    allowed = seg_keys[...] == seg_queries[...]
    scale = 1.0 / math.sqrt(HD)
    for half in range(2):
        lanes = slice(half * HD, (half + 1) * HD)
        queries, key_rows, value_rows = q_ref[:, lanes], k_ref[:, lanes], v_ref[:, lanes]
        grads = grad_ref[:, lanes]
        products = grads.astype(F32) * out_ref[:, lanes].astype(F32)
        inner = jnp.sum(products.T, axis=0, keepdims=True)
        scores = across(key_rows, queries) * scale
        probs = jnp.where(allowed, jnp.exp(scores - lse_ref[0, half : half + 1, :]), 0.0)
        dv_ref[:, lanes] = jnp.dot(probs.astype(BF16), grads, preferred_element_type=F32).astype(BF16)
        grad_probs = across(value_rows, grads)
        grad_scores = (probs * (grad_probs - inner) * scale).astype(BF16)
        dk_ref[:, lanes] = jnp.dot(grad_scores, queries, preferred_element_type=F32).astype(BF16)
        dq_ref[:, lanes] = down(key_rows, grad_scores).T.astype(BF16)


def attend_back(queries_keys, value_rows, attended, grads, log_totals, segments):
    rows, width = value_rows.shape
    pairs = width // (2 * HD)
    block = (rows, 2 * HD)
    plain = pl.BlockSpec(block, lambda i: (0, i))
    return pl.pallas_call(
        attend_back_kernel,
        grid=(pairs,),
        in_specs=[
            plain,
            pl.BlockSpec(block, lambda i: (0, pairs + i)),
            plain,
            plain,
            plain,
            pl.BlockSpec((1, 8, rows), lambda i: (i, 0, 0)),
            pl.BlockSpec((rows, 1), lambda i: (0, 0)),
            pl.BlockSpec((1, rows), lambda i: (0, 0)),
        ],
        out_specs=[plain] * 3,
        out_shape=[jax.ShapeDtypeStruct((rows, width), BF16)] * 3,
        cost_estimate=pl.CostEstimate(
            flops=40 * rows * rows * width, bytes_accessed=20 * rows * width, transcendentals=6 * rows * rows
        ),
        name="attend_back",
    )(
        queries_keys,
        queries_keys,
        value_rows,
        attended,
        grads,
        log_totals,
        segments,
        segments.reshape(1, rows),
    )


def blocks_of(left, right, low, high, rows):
    turned = left[low:high].T

    def part(index):
        chunk = lax.dynamic_slice_in_dim(turned, index * rows, rows, 0)
        return jnp.dot(chunk, right, preferred_element_type=F32)

    return part


def joined(parts):
    return lambda index: jnp.concatenate([part(index) for part in parts], axis=1)


STREAMS = ((0, IMG_DEV), (IMG_DEV, ROWS))


def per_device(
    image_in,
    text_in,
    condition,
    ranges,
    mod_weight,
    qkv_weight,
    out_weight,
    up_weight,
    down_weight,
    image_cot,
    text_cot,
):
    members, segments = slot_table(ranges, IMG_DEV, TXT_DEV)
    slot_ones = jnp.concatenate(members, axis=1)
    col_width = image_in.shape[1]
    ff_width = up_weight.shape[3]
    half_ff = ff_width // 2
    row_count = qkv_weight.shape[1]
    size = lax.axis_size("row")
    ring = Ring(size) if size <= RING_LIMIT else None

    qkv_local, out_local = qkv_weight[0], out_weight[0]
    up_local, down_local = up_weight[0], down_weight[0]
    first_pieces = [
        [
            jnp.concatenate([qkv_local[:, way, 0], qkv_local[:, way, 1]], axis=1),
            jnp.concatenate([qkv_local[:, way, 2], out_local[:, way]], axis=1),
        ]
        for way in range(2)
    ]
    halves = lambda weight: [[weight[:, way, :half_ff], weight[:, way, half_ff:]] for way in range(2)]

    def late(arrivals, back=2):
        return None if arrivals is None else [seen[-back] for seen in arrivals]

    silu_cond = jax.nn.silu(condition.astype(F32)).astype(BF16)
    mod_terms = jnp.einsum("sd,ldxkf->slxkf", silu_cond, mod_weight, preferred_element_type=F32)
    mod_mine = exchange_sum(ring, mod_terms)

    first, arrivals = gather_pieces(ring, first_pieces, None)
    up_whole, arrivals = gather_pieces(ring, halves(up_local), late(arrivals))
    down_whole, arrivals = gather_pieces(ring, halves(down_local), late(arrivals))
    after_gather = late(arrivals)
    qk_whole = [first[way][0] for way in range(2)]
    v_whole = [first[way][1][:, :col_width] for way in range(2)]
    out_whole = [first[way][1][:, col_width:] for way in range(2)]

    def wide_dot(left, whole):
        return jnp.concatenate([stream_dot(left, whole[0][part], whole[1][part]) for part in range(2)], axis=1)

    def wide_back(left, whole):
        return stream_dot_back(left[:, :half_ff], whole[0][0], whole[1][0]) + stream_dot_back(
            left[:, half_ff:], whole[0][1], whole[1][1]
        )

    hidden = jnp.concatenate([image_in, text_in], axis=0).astype(F32)
    mods = [row_mod(members, mod_mine, part_no) for part_no in range(6)]
    normed_one, scaling_one = normalize(hidden)
    modulated_one = (normed_one * (1.0 + mods[1]) + mods[0]).astype(BF16)
    gathered_one = gather_features(modulated_one)
    queries_keys = stream_dot(gathered_one, *qk_whole).astype(BF16)
    value_rows = stream_dot(gathered_one, *v_whole).astype(BF16)
    mixed, log_totals = attend(queries_keys, value_rows, segments)
    branch_one = scatter_features(stream_dot_back(mixed, *out_whole))
    midway = hidden + mods[2] * branch_one
    normed_two, scaling_two = normalize(midway)
    modulated_two = (normed_two * (1.0 + mods[4]) + mods[3]).astype(BF16)
    gathered_two = gather_features(modulated_two)
    lifted = wide_dot(gathered_two, up_whole)
    activated = jax.nn.gelu(lifted, approximate=True).astype(BF16)
    branch_two = scatter_features(wide_back(activated, down_whole))
    hidden = midway + mods[5] * branch_two
    image_out = hidden[:IMG_DEV]
    text_out = hidden[IMG_DEV:]

    grad_hidden = jnp.concatenate([image_cot, text_cot], axis=0).astype(F32)
    grad_branch_two = (grad_hidden * mods[5]).astype(BF16)
    gate_two_rows = grad_hidden * branch_two
    grad_full_two = gather_features(grad_branch_two)
    down_parts = [
        [
            blocks_of(grad_full_two, activated[low:high, start : start + half_ff], low, high, row_count)
            for start in (0, half_ff)
        ]
        for low, high in STREAMS
    ]
    grads_down, arrivals = scatter_pieces(ring, down_parts, after_gather)
    grad_act = wide_dot(grad_full_two, down_whole)
    grad_lifted = (grad_act * gelu_slope(lifted)).astype(BF16)
    up_parts = [
        [
            blocks_of(gathered_two, grad_lifted[low:high, start : start + half_ff], low, high, row_count)
            for start in (0, half_ff)
        ]
        for low, high in STREAMS
    ]
    grads_up, arrivals = scatter_pieces(ring, up_parts, late(arrivals))
    grad_mod_two = scatter_features(wide_back(grad_lifted, up_whole))
    scale_two_rows = grad_mod_two * normed_two
    grad_hidden = grad_hidden + norm_back(grad_mod_two * (1.0 + mods[4]), normed_two, scaling_two)
    grad_branch_one = (grad_hidden * mods[2]).astype(BF16)
    gate_one_rows = grad_hidden * branch_one
    grad_full_one = gather_features(grad_branch_one)
    grad_mixed = stream_dot(grad_full_one, *out_whole).astype(BF16)
    grad_q, grad_k, grad_v = attend_back(queries_keys, value_rows, mixed, grad_mixed, log_totals, segments)
    grad_qk = jnp.concatenate([grad_q, grad_k], axis=1)
    first_parts = [
        [
            blocks_of(gathered_one, grad_qk[low:high], low, high, row_count),
            joined(
                [
                    blocks_of(gathered_one, grad_v[low:high], low, high, row_count),
                    blocks_of(grad_full_one, mixed[low:high], low, high, row_count),
                ]
            ),
        ]
        for low, high in STREAMS
    ]
    grads_first, _ = scatter_pieces(ring, first_parts, late(arrivals))
    grad_mod_one = scatter_features(stream_dot_back(grad_qk, *qk_whole) + stream_dot_back(grad_v, *v_whole))
    scale_one_rows = grad_mod_one * normed_one
    grad_hidden = grad_hidden + norm_back(grad_mod_one * (1.0 + mods[1]), normed_one, scaling_one)
    rows_list = [
        grad_mod_one,
        scale_one_rows,
        gate_one_rows,
        grad_mod_two,
        scale_two_rows,
        gate_two_rows,
    ]
    slot_grads = jnp.stack([slot_sums(slot_ones, rows) for rows in rows_list], axis=2)
    mod_all = spread_all(ring, slot_grads[:, None])
    grad_mod = jnp.einsum("sd,slxkf->ldxkf", silu_cond.astype(F32), mod_all, precision=HIGHEST)
    cond_part = jnp.einsum("slxkf,ldxkf->sd", mod_all, mod_weight.astype(F32), precision=HIGHEST)
    cond_total = lax.psum(cond_part, "col")
    grad_cond = cond_total * silu_slope(condition.astype(F32))

    def stacked(grads):
        return jnp.stack([jnp.concatenate(parts, axis=1) for parts in grads], axis=1)

    grad_qkv = jnp.stack(
        [
            jnp.stack(
                [parts[0][:, :col_width], parts[0][:, col_width:], parts[1][:, :col_width]],
                axis=1,
            )
            for parts in grads_first
        ],
        axis=1,
    )
    grad_out = jnp.stack([parts[1][:, col_width:] for parts in grads_first], axis=1)
    return (
        image_out,
        text_out,
        grad_hidden[:IMG_DEV],
        grad_hidden[IMG_DEV:],
        grad_cond,
        grad_mod,
        grad_qkv[None],
        grad_out[None],
        stacked(grads_up)[None],
        stacked(grads_down)[None],
    )


def solution(mesh):
    return jax.shard_map(
        per_device,
        mesh=mesh,
        in_specs=(
            P("row", "col"),
            P("row", "col"),
            P(None, "row"),
            P("row", None),
            P(None, "row", None, None, "col"),
            P(None, "row", None, None, "col"),
            P(None, "row", None, "col"),
            P(None, "row", None, "col"),
            P(None, "row", None, "col"),
            P("row", "col"),
            P("row", "col"),
        ),
        out_specs=(
            P("row", "col"),
            P("row", "col"),
            P("row", "col"),
            P("row", "col"),
            P(None, "row"),
            P(None, "row", None, None, "col"),
            P(None, "row", None, None, "col"),
            P(None, "row", None, "col"),
            P(None, "row", None, "col"),
            P(None, "row", None, "col"),
        ),
        check_vma=False,
    )
```

```python
import functools
import math

import jax
import jax.numpy as jnp
from jax import lax
from jax.experimental import pallas as pl
from jax.experimental.pallas import tpu as pltpu
from jax.sharding import PartitionSpec as P

D = 1536
IMG_DEV = 256
HD = 64
TXT_DEV = 308
ROWS = IMG_DEV + TXT_DEV

EPSILON = 1e-06
HIGHEST = lax.Precision.HIGHEST
BF16 = jnp.bfloat16
F32 = jnp.float32
RING_LIMIT = 8


class Ring:
    def __init__(self, count):
        order = list(range(0, count, 2)) + list(range(count - 1, 0, -2))
        forward = [(order[k], order[(k + 1) % count]) for k in range(count)]
        self.count = count
        self.perms = (forward, [(target, source) for source, target in forward])
        me = lax.axis_index("row")
        self.me = me
        self.place = jnp.where((me & 1) == 0, me >> 1, count - 1 - (me >> 1))
        self.owners = {}

    def wrap(self, value):
        if self.count & (self.count - 1) == 0:
            return value & (self.count - 1)
        return lax.rem(value + self.count, self.count)

    def owner(self, way, step):
        shift = (-step if way == 0 else step) % self.count
        if shift not in self.owners:
            spot = self.wrap(self.place + shift) if shift else self.place
            self.owners[shift] = jnp.where(
                spot < self.count // 2, spot << 1, 2 * self.count - 1 - (spot << 1)
            )
        return self.owners[shift]


def after(value, *gates):
    gates = [gate for gate in gates if gate is not None]
    return lax.optimization_barrier((value, *gates))[0] if gates else value


class Gather:
    def __init__(self, ring, pieces):
        self.ring, self.held, self.step = ring, [list(group) for group in pieces], 0
        if ring is None:
            return
        self.built = None

    def start(self, behind):
        self.built = []
        for way, group in enumerate(self.held):
            built = []
            for number, piece in enumerate(group):
                zero = jnp.zeros((), piece.dtype)
                if behind is not None:
                    gate = behind.last(way, number)
                    zero, piece = after(zero, gate), after(piece, gate)
                    group[number] = piece
                rows = piece.shape[0]
                whole = jnp.broadcast_to(zero, (rows * self.ring.count, piece.shape[1]))
                built.append(lax.dynamic_update_slice(whole, piece, (self.ring.owner(way, 0) * rows, 0)))
            self.built.append(built)

    def round(self, *gates, behind=None):
        if self.ring is None:
            return
        if self.step == 0:
            self.start(behind)
        self.step += 1
        for way, group in enumerate(self.held):
            for number, piece in enumerate(group):
                held = gates if number == len(group) - 1 else ()
                piece = lax.ppermute(after(piece, *held), "row", self.ring.perms[way])
                group[number] = piece
                rows = piece.shape[0]
                self.built[way][number] = lax.dynamic_update_slice(
                    self.built[way][number], piece, (self.ring.owner(way, self.step) * rows, 0)
                )

    def last(self, way=0, number=0):
        return None if self.ring is None else self.held[way][number]

    def whole(self, way, number):
        if self.ring is None:
            return lax.all_gather(self.held[way][number], "row", axis=0, tiled=True)
        return self.built[way][number]


class Scatter:
    def __init__(self, ring, pieces):
        self.ring, self.pieces, self.step = ring, pieces, 0
        if ring is None:
            return
        self.totals = [[self.block(way, part) for part in group] for way, group in enumerate(pieces)]
        self.came = [[None for _ in group] for group in pieces]

    def block(self, way, part):
        rows = part.shape[0] // self.ring.count
        return lax.dynamic_slice_in_dim(part, self.ring.owner(way, self.step + 1) * rows, rows, 0)

    def round(self, *gates, behind=None):
        if self.ring is None:
            return
        self.step += 1
        for way, group in enumerate(self.pieces):
            for number, part in enumerate(group):
                ahead = None if behind is None else behind.last(way, number)
                held = gates if number == len(group) - 1 else ()
                total = after(self.totals[way][number].astype(BF16), ahead, *held)
                came = lax.ppermute(total, "row", self.ring.perms[way])
                self.came[way][number] = came
                own = self.block(way, after(part, came))
                self.totals[way][number] = came.astype(F32) + own.astype(F32)

    def last(self, way=0, number=0):
        return None if self.ring is None else self.came[way][number]

    def result(self, way, number):
        if self.ring is not None:
            return self.totals[way][number]
        return sum_blocks(self.pieces[way][number])


def sum_blocks(part):
    return lax.psum_scatter(part, "row", scatter_dimension=0, tiled=True).astype(F32)


def exchange_sum(ring, values, first):
    if ring is None:
        return lax.psum_scatter(values, "row", scatter_dimension=0, tiled=True)
    bit = ring.count // 2
    rounds = 0
    while bit:
        high = (ring.me & bit) != 0
        half = values.shape[0] // 2
        away = jnp.where(high, values[:half], values[half:])
        came = lax.ppermute(away, "row", [(index, index ^ bit) for index in range(ring.count)])
        values = jnp.where(high, values[half:], values[:half]) + came
        bit //= 2
        if rounds < 2:
            first.round()
            values = after(values, first.last())
            rounds += 1
    return values


def spread_all(ring, values):
    if ring is None:
        return lax.all_gather(values, "row", axis=0, tiled=True)
    bit = 1
    while bit < ring.count:
        high = (ring.me & bit) != 0
        came = lax.ppermute(values, "row", [(index, index ^ bit) for index in range(ring.count)])
        values = jnp.concatenate([jnp.where(high, came, values), jnp.where(high, values, came)], axis=0)
        bit *= 2
    return values


def swaps(bit):
    return [(index, index ^ bit) for index in range(4)]


def gather_features(values):
    if lax.axis_size("col") != 4:
        return lax.all_gather(values, "col", axis=1, tiled=True)
    me = lax.axis_index("col")
    odd, high = (me & 1) == 1, (me & 2) == 2
    far = lax.ppermute(values, "col", swaps(2))
    near = lax.ppermute(values, "col", swaps(1))
    diagonal = lax.ppermute(far, "col", swaps(1))
    mine = [jnp.where(odd, near, values), jnp.where(odd, values, near)]
    other = [jnp.where(odd, diagonal, far), jnp.where(odd, far, diagonal)]
    return jnp.concatenate(
        [jnp.where(high, other[0], mine[0]), jnp.where(high, other[1], mine[1])]
        + [jnp.where(high, mine[0], other[0]), jnp.where(high, mine[1], other[1])],
        axis=1,
    )


def scatter_features(values):
    if lax.axis_size("col") != 4:
        return lax.psum_scatter(values, "col", scatter_dimension=1, tiled=True), None, None
    me = lax.axis_index("col")
    odd, high = (me & 1) == 1, (me & 2) == 2
    width = values.shape[1] // 4
    blocks = [values[:, index * width : (index + 1) * width] for index in range(4)]
    away = jnp.concatenate([jnp.where(odd, blocks[0], blocks[1]), jnp.where(odd, blocks[2], blocks[3])], axis=1)
    step = (away.shape[0] // 4 + 15) // 8 * 8
    cuts = [min(index * step, away.shape[0]) for index in range(5)]
    chunks = [lax.ppermute(away[low:high_row], "col", swaps(1)) for low, high_row in zip(cuts, cuts[1:])]
    came = jnp.concatenate(chunks, axis=0)
    low_sum = jnp.where(odd, blocks[1], blocks[0]) + came[:, :width]
    high_sum = jnp.where(odd, blocks[3], blocks[2]) + came[:, width:]
    last = lax.ppermute(jnp.where(high, low_sum, high_sum).astype(BF16), "col", swaps(2))
    return jnp.where(high, high_sum, low_sum) + last.astype(F32), chunks[-1], last


def slot_table(lengths, image_rows, text_rows):
    slots = lengths.shape[0]
    tables = []
    segments = []
    for column, amount in ((0, image_rows), (1, text_rows)):
        places = jnp.arange(amount, dtype=jnp.int32)[:, None]
        low = jnp.zeros((), jnp.int32)
        segment = jnp.full((amount, 1), slots, jnp.int32)
        for slot in range(slots):
            high = low + lengths[slot, column]
            inside = (places >= low) & (places < high)
            tables.append(inside.astype(F32))
            segment = jnp.where(inside, slot, segment)
            low = high
        segments.append(segment)
    pairs = [jnp.concatenate([tables[slot], tables[slots + slot]], axis=0) for slot in range(slots)]
    return pairs, jnp.concatenate(segments, axis=0)


def stream_dot(left, right_image, right_text):
    upper = jnp.dot(left[:IMG_DEV], right_image, preferred_element_type=F32)
    lower = jnp.dot(left[IMG_DEV:], right_text, preferred_element_type=F32)
    return jnp.concatenate([upper, lower], axis=0)


def stream_dot_back(left, right_image, right_text):
    return stream_dot(left, right_image.T, right_text.T)


def row_mod(members, mod_mine, component):
    streams = []
    for stream, (low, high) in enumerate(((0, IMG_DEV), (IMG_DEV, ROWS))):
        total = None
        for slot, member in enumerate(members):
            term = member[low:high] * mod_mine[slot, 0, stream, component][None, :]
            total = term if total is None else total + term
        streams.append(total)
    return jnp.concatenate(streams, axis=0)


def slot_sums(slot_ones, rows):
    upper = jnp.dot(slot_ones[:IMG_DEV].T, rows[:IMG_DEV], precision=HIGHEST)
    lower = jnp.dot(slot_ones[IMG_DEV:].T, rows[IMG_DEV:], precision=HIGHEST)
    return jnp.stack([upper, lower], axis=1)


def col_sum(values):
    if lax.axis_size("col") != 4:
        return lax.psum(values, "col")
    values = values + lax.ppermute(values, "col", swaps(1))
    return values + lax.ppermute(values, "col", swaps(2))


def feature_sums(first, second, *gates):
    sums = jnp.stack([jnp.sum(first, axis=1), jnp.sum(second, axis=1)], axis=0)
    sums = col_sum(after(sums, *gates))
    return sums[0], sums[1]


def normalize(hidden, *gates):
    totals, squares = feature_sums(hidden, hidden * hidden, *gates)
    center = totals / D
    spread = squares / D - center * center
    scaling = lax.rsqrt(spread + EPSILON)
    return ((hidden - center[:, None]) * scaling[:, None], scaling[:, None])


def norm_back(grad_hat, normed, scaling):
    first, second = feature_sums(grad_hat, grad_hat * normed)
    return scaling * (grad_hat - first[:, None] / D - normed * (second[:, None] / D))


def gelu_slope(value):
    coeff = math.sqrt(2.0 / math.pi)
    tangent = jnp.tanh(coeff * (value + 0.044715 * value * value * value))
    return 0.5 * (1.0 + tangent) + 0.5 * value * (1.0 - tangent * tangent) * coeff * (
        1.0 + 3.0 * 0.044715 * value * value
    )


def silu_slope(value):
    sigma = jax.nn.sigmoid(value)
    return sigma * (1.0 + value * (1.0 - sigma))


def across(left, right):
    return lax.dot_general(left, right, (((1,), (1,)), ((), ())), preferred_element_type=F32)


def down(left, right):
    return lax.dot_general(left, right, (((0,), (0,)), ((), ())), preferred_element_type=F32)


def attend_kernel(q_ref, k_ref, v_ref, seg_keys, seg_queries, out_ref, lse_ref):
    allowed = seg_keys[...] == seg_queries[...]
    for half in range(2):
        lanes = slice(half * HD, (half + 1) * HD)
        queries, key_rows, value_rows = q_ref[:, lanes], k_ref[:, lanes], v_ref[:, lanes]
        scores = jnp.where(allowed, across(key_rows, queries) * (1.0 / math.sqrt(HD)), -jnp.inf)
        highest = jnp.max(scores, axis=0, keepdims=True)
        powers = jnp.exp(scores - highest)
        total = jnp.sum(powers, axis=0, keepdims=True)
        weights = (powers * (1.0 / total)).astype(BF16)
        out_ref[:, lanes] = down(value_rows, weights).T.astype(BF16)
        lse_ref[0, half : half + 1, :] = highest + jnp.log(total)


def attend(queries_keys, value_rows, segments):
    rows, width = value_rows.shape
    pairs = width // (2 * HD)
    block = (rows, 2 * HD)
    return pl.pallas_call(
        attend_kernel,
        grid=(pairs,),
        in_specs=[
            pl.BlockSpec(block, lambda i: (0, i)),
            pl.BlockSpec(block, lambda i: (0, pairs + i)),
            pl.BlockSpec(block, lambda i: (0, i)),
            pl.BlockSpec((rows, 1), lambda i: (0, 0)),
            pl.BlockSpec((1, rows), lambda i: (0, 0)),
        ],
        out_specs=[
            pl.BlockSpec(block, lambda i: (0, i)),
            pl.BlockSpec((1, 8, rows), lambda i: (i, 0, 0)),
        ],
        out_shape=[
            jax.ShapeDtypeStruct((rows, width), BF16),
            jax.ShapeDtypeStruct((pairs, 8, rows), F32),
        ],
        cost_estimate=pl.CostEstimate(
            flops=20 * rows * rows * width, bytes_accessed=10 * rows * width, transcendentals=6 * rows * rows
        ),
        name="attend",
    )(queries_keys, queries_keys, value_rows, segments, segments.reshape(1, rows))


def attend_back_kernel(
    q_ref, k_ref, v_ref, out_ref, grad_ref, lse_ref, seg_keys, seg_queries, dq_ref, dk_ref, dv_ref
):
    allowed = seg_keys[...] == seg_queries[...]
    scale = 1.0 / math.sqrt(HD)
    for half in range(2):
        lanes = slice(half * HD, (half + 1) * HD)
        queries, key_rows, value_rows = q_ref[:, lanes], k_ref[:, lanes], v_ref[:, lanes]
        grads = grad_ref[:, lanes]
        products = grads.astype(F32) * out_ref[:, lanes].astype(F32)
        inner = jnp.sum(products.T, axis=0, keepdims=True)
        scores = across(key_rows, queries) * scale
        probs = jnp.where(allowed, jnp.exp(scores - lse_ref[0, half : half + 1, :]), 0.0)
        dv_ref[:, lanes] = jnp.dot(probs.astype(BF16), grads, preferred_element_type=F32).astype(BF16)
        grad_probs = across(value_rows, grads)
        grad_scores = (probs * (grad_probs - inner) * scale).astype(BF16)
        dk_ref[:, lanes] = jnp.dot(grad_scores, queries, preferred_element_type=F32).astype(BF16)
        dq_ref[:, lanes] = down(key_rows, grad_scores).T.astype(BF16)


def attend_back(queries_keys, value_rows, attended, grads, log_totals, segments):
    rows, width = value_rows.shape
    pairs = width // (2 * HD)
    block = (rows, 2 * HD)
    plain = pl.BlockSpec(block, lambda i: (0, i))
    return pl.pallas_call(
        attend_back_kernel,
        grid=(pairs,),
        in_specs=[
            plain,
            pl.BlockSpec(block, lambda i: (0, pairs + i)),
            plain,
            plain,
            plain,
            pl.BlockSpec((1, 8, rows), lambda i: (i, 0, 0)),
            pl.BlockSpec((rows, 1), lambda i: (0, 0)),
            pl.BlockSpec((1, rows), lambda i: (0, 0)),
        ],
        out_specs=[plain] * 3,
        out_shape=[jax.ShapeDtypeStruct((rows, width), BF16)] * 3,
        cost_estimate=pl.CostEstimate(
            flops=40 * rows * rows * width, bytes_accessed=20 * rows * width, transcendentals=6 * rows * rows
        ),
        name="attend_back",
    )(
        queries_keys,
        queries_keys,
        value_rows,
        attended,
        grads,
        log_totals,
        segments,
        segments.reshape(1, rows),
    )


def part_of(left, right, low, high):
    return jnp.einsum("nk,nf->kf", left[low:high], right[low:high], preferred_element_type=F32).astype(BF16)


STREAMS = ((0, IMG_DEV), (IMG_DEV, ROWS))


def per_device(
    image_in,
    text_in,
    condition,
    ranges,
    mod_weight,
    qkv_weight,
    out_weight,
    up_weight,
    down_weight,
    image_cot,
    text_cot,
):
    members, segments = slot_table(ranges, IMG_DEV, TXT_DEV)
    slot_ones = jnp.concatenate(members, axis=1)
    col_width = image_in.shape[1]
    ff_width = up_weight.shape[3]
    half_ff = ff_width // 2
    size = lax.axis_size("row")
    ring = Ring(size) if size <= RING_LIMIT else None

    qkv_local, out_local = qkv_weight[0], out_weight[0]
    up_local, down_local = up_weight[0], down_weight[0]
    first_pieces = [
        [
            jnp.concatenate([qkv_local[:, way, 0], qkv_local[:, way, 1]], axis=1),
            jnp.concatenate([qkv_local[:, way, 2], out_local[:, way]], axis=1),
        ]
        for way in range(2)
    ]
    halves = lambda weight: [[weight[:, way, :half_ff], weight[:, way, half_ff:]] for way in range(2)]
    first, up, last = (
        Gather(ring, first_pieces),
        Gather(ring, halves(up_local)),
        Gather(ring, halves(down_local)),
    )

    def part_dot(left, source, part):
        return stream_dot(left, source.whole(0, part), source.whole(1, part))

    def part_back(left, source, part):
        return stream_dot_back(left, source.whole(0, part), source.whole(1, part))

    silu_cond = jax.nn.silu(condition.astype(F32)).astype(BF16)
    mod_terms = jnp.einsum("sd,ldxkf->slxkf", silu_cond, mod_weight, preferred_element_type=F32)
    first.round()
    mod_mine = exchange_sum(ring, mod_terms, first)
    hidden = jnp.concatenate([image_in, text_in], axis=0).astype(F32)
    normed_one, scaling_one = normalize(hidden, first.last())
    mods = [row_mod(members, mod_mine, part_no) for part_no in range(6)]
    modulated_one = (normed_one * (1.0 + mods[1]) + mods[0]).astype(BF16)
    gathered_one = gather_features(modulated_one)
    while first.step < 3:
        first.round()
    grad_hidden = jnp.concatenate([image_cot, text_cot], axis=0).astype(F32)
    grad_branch_two = (grad_hidden * mods[5]).astype(BF16)
    first.round()
    first.round(modulated_one)
    first.round(gathered_one)
    first.round()
    up.round(behind=first)

    qk_whole = [first.whole(way, 0) for way in range(2)]
    v_whole = [first.whole(way, 1)[:, :col_width] for way in range(2)]
    out_whole = [first.whole(way, 1)[:, col_width:] for way in range(2)]
    queries_keys = stream_dot(gathered_one, *qk_whole).astype(BF16)
    value_rows = stream_dot(after(gathered_one, up.last()), *v_whole).astype(BF16)
    up.round()
    mixed, log_totals = attend(queries_keys, after(value_rows, up.last()), segments)
    up.round()
    branch_one, stage, stage_two = scatter_features(stream_dot_back(mixed, *out_whole))
    grad_full_two = gather_features(after(grad_branch_two, up.last()))
    up.round(mixed)
    up.round(stage)
    midway = hidden + mods[2] * branch_one
    normed_two, scaling_two = normalize(midway)
    modulated_two = (normed_two * (1.0 + mods[4]) + mods[3]).astype(BF16)
    up.round(stage_two)
    up.round(modulated_two)
    gathered_two = gather_features(modulated_two)
    last.round(behind=up)
    last.round()
    lifted, activated, down_parts = [], [], [[], []]
    for part in range(2):
        lifted.append(part_dot(after(gathered_two, last.last()), up, part))
        activated.append(jax.nn.gelu(lifted[part], approximate=True).astype(BF16))
        last.round(activated[part] if part else gathered_two)
    for part in range(2):
        given = after(grad_full_two, last.last())
        for way, (low, high) in enumerate(STREAMS):
            down_parts[way].append(part_of(given, activated[part], low, high))
        last.round(down_parts[1][part])
    last.round()

    down_sums = Scatter(ring, down_parts)
    down_sums.round(behind=last)
    grad_lifted = []
    for part in range(2):
        grad_act = part_dot(after(grad_full_two, down_sums.last()), last, part)
        grad_lifted.append((grad_act * gelu_slope(lifted[part])).astype(BF16))
        down_sums.round(grad_lifted[part] if part else None)
    lower_part = part_back(after(grad_lifted[0], down_sums.last()), up, 0)
    down_sums.round()
    grad_mod_two, stage, stage_two = scatter_features(
        lower_part + part_back(after(grad_lifted[1], down_sums.last()), up, 1)
    )
    down_sums.round()
    up_parts = [[], []]
    for part in range(2):
        given = after(gathered_two, down_sums.last())
        for way, (low, high) in enumerate(STREAMS):
            up_parts[way].append(part_of(given, grad_lifted[part], low, high))
        down_sums.round(up_parts[1][part], stage)
    up_sums = Scatter(ring, up_parts)
    up_sums.round(stage_two, behind=down_sums)
    scale_two_rows = grad_mod_two * normed_two
    grad_hidden_two = grad_hidden
    grad_hidden = grad_hidden + norm_back(grad_mod_two * (1.0 + mods[4]), normed_two, scaling_two)
    grad_branch_one = (grad_hidden * mods[2]).astype(BF16)
    gate_one_rows = grad_hidden * branch_one
    lower_part = part_back(after(activated[0], up_sums.last()), last, 0)
    up_sums.round(grad_branch_one)
    grad_full_one = gather_features(grad_branch_one)
    branch_two, _, stage_far = scatter_features(
        lower_part + part_back(after(activated[1], up_sums.last()), last, 1)
    )
    hidden = midway + mods[5] * branch_two
    image_out = hidden[:IMG_DEV]
    text_out = hidden[IMG_DEV:]
    gate_two_rows = grad_hidden_two * branch_two
    up_sums.round()
    grad_mixed = stream_dot(after(grad_full_one, up_sums.last()), *out_whole).astype(BF16)
    up_sums.round(grad_mixed)
    grad_q, grad_k, grad_v = attend_back(
        queries_keys, value_rows, mixed, after(grad_mixed, up_sums.last()), log_totals, segments
    )
    grad_qk = jnp.concatenate([grad_q, grad_k], axis=1)
    up_sums.round()
    qk_parts = [part_of(gathered_one, after(grad_qk, up_sums.last()), low, high) for low, high in STREAMS]
    up_sums.round(grad_v, stage_far)
    given = after(gathered_one, up_sums.last())
    other_parts = [
        jnp.concatenate([part_of(given, grad_v, low, high), part_of(grad_full_one, mixed, low, high)], axis=1)
        for low, high in STREAMS
    ]
    up_sums.round(qk_parts[1])
    first_sums = Scatter(ring, [[qk_parts[way], other_parts[way]] for way in range(2)])
    first_sums.round(behind=up_sums)
    grad_mod_one, stage, stage_two = scatter_features(
        stream_dot_back(after(grad_qk, first_sums.last()), *qk_whole) + stream_dot_back(grad_v, *v_whole)
    )
    first_sums.round()
    first_sums.round(stage)
    scale_one_rows = grad_mod_one * normed_one
    grad_hidden = grad_hidden + norm_back(grad_mod_one * (1.0 + mods[1]), normed_one, scaling_one)
    rows_list = [
        grad_mod_one,
        scale_one_rows,
        gate_one_rows,
        grad_mod_two,
        scale_two_rows,
        gate_two_rows,
    ]
    slot_grads = jnp.stack([slot_sums(slot_ones, rows) for rows in rows_list], axis=2)
    first_sums.round(stage_two)
    first_sums.round(slot_grads)
    mod_all = spread_all(ring, slot_grads[:, None])
    grad_mod = jnp.einsum("sd,slxkf->ldxkf", silu_cond.astype(F32), mod_all, precision=HIGHEST)
    cond_part = jnp.einsum("slxkf,ldxkf->sd", mod_all, mod_weight.astype(F32), precision=HIGHEST)
    cond_total = col_sum(cond_part)
    grad_cond = cond_total * silu_slope(condition.astype(F32))
    first_sums.round(mod_all)
    first_sums.round(cond_total)
    gather_sums = lambda sums: [[sums.result(way, number) for number in range(2)] for way in range(2)]
    grads_first, grads_up, grads_down = (gather_sums(sums) for sums in (first_sums, up_sums, down_sums))

    def stacked(grads):
        return jnp.stack([jnp.concatenate(parts, axis=1) for parts in grads], axis=1)

    grad_qkv = jnp.stack(
        [
            jnp.stack(
                [parts[0][:, :col_width], parts[0][:, col_width:], parts[1][:, :col_width]],
                axis=1,
            )
            for parts in grads_first
        ],
        axis=1,
    )
    grad_out = jnp.stack([parts[1][:, col_width:] for parts in grads_first], axis=1)
    return (
        image_out,
        text_out,
        grad_hidden[:IMG_DEV],
        grad_hidden[IMG_DEV:],
        grad_cond,
        grad_mod,
        grad_qkv[None],
        grad_out[None],
        stacked(grads_up)[None],
        stacked(grads_down)[None],
    )


def solution(mesh):
    return jax.shard_map(
        per_device,
        mesh=mesh,
        in_specs=(
            P("row", "col"),
            P("row", "col"),
            P(None, "row"),
            P("row", None),
            P(None, "row", None, None, "col"),
            P(None, "row", None, None, "col"),
            P(None, "row", None, "col"),
            P(None, "row", None, "col"),
            P(None, "row", None, "col"),
            P("row", "col"),
            P("row", "col"),
        ),
        out_specs=(
            P("row", "col"),
            P("row", "col"),
            P("row", "col"),
            P("row", "col"),
            P(None, "row"),
            P(None, "row", None, None, "col"),
            P(None, "row", None, None, "col"),
            P(None, "row", None, "col"),
            P(None, "row", None, "col"),
            P(None, "row", None, "col"),
        ),
        check_vma=False,
    )
```

```python
import functools
import math

import jax
import jax.numpy as jnp
from jax import lax
from jax.experimental import pallas as pl
from jax.experimental.pallas import tpu as pltpu
from jax.sharding import PartitionSpec as P

D = 1536
IMG_DEV = 256
HD = 64
TXT_DEV = 308
ROWS = IMG_DEV + TXT_DEV

EPSILON = 1e-06
HIGHEST = lax.Precision.HIGHEST
BF16 = jnp.bfloat16
F32 = jnp.float32
RING_LIMIT = 8


class Ring:
    def __init__(self, count):
        order = list(range(0, count, 2)) + list(range(count - 1, 0, -2))
        forward = [(order[k], order[(k + 1) % count]) for k in range(count)]
        self.count = count
        self.perms = (forward, [(target, source) for source, target in forward])
        me = lax.axis_index("row")
        self.me = me
        self.place = jnp.where((me & 1) == 0, me >> 1, count - 1 - (me >> 1))
        self.owners = {}

    def wrap(self, value):
        if self.count & (self.count - 1) == 0:
            return value & (self.count - 1)
        return lax.rem(value + self.count, self.count)

    def owner(self, way, step):
        shift = (-step if way == 0 else step) % self.count
        if shift not in self.owners:
            spot = self.wrap(self.place + shift) if shift else self.place
            self.owners[shift] = jnp.where(
                spot < self.count // 2, spot << 1, 2 * self.count - 1 - (spot << 1)
            )
        return self.owners[shift]


def after(value, *gates):
    gates = [gate for gate in gates if gate is not None]
    return lax.optimization_barrier((value, *gates))[0] if gates else value


class Gather:
    def __init__(self, ring, pieces):
        self.ring, self.held, self.step = ring, [list(group) for group in pieces], 0
        if ring is None:
            return
        self.built = None

    def start(self, behind):
        self.built = []
        for way, group in enumerate(self.held):
            built = []
            for number, piece in enumerate(group):
                zero = jnp.zeros((), piece.dtype)
                if behind is not None:
                    gate = behind.last(way, number)
                    zero, piece = after(zero, gate), after(piece, gate)
                    group[number] = piece
                rows = piece.shape[0]
                whole = jnp.broadcast_to(zero, (rows * self.ring.count, piece.shape[1]))
                built.append(lax.dynamic_update_slice(whole, piece, (self.ring.owner(way, 0) * rows, 0)))
            self.built.append(built)

    def round(self, *gates, behind=None):
        if self.ring is None:
            return
        if self.step == 0:
            self.start(behind)
        self.step += 1
        for way, group in enumerate(self.held):
            for number, piece in enumerate(group):
                held = gates if number == len(group) - 1 else ()
                piece = lax.ppermute(after(piece, *held), "row", self.ring.perms[way])
                group[number] = piece
                rows = piece.shape[0]
                self.built[way][number] = lax.dynamic_update_slice(
                    self.built[way][number], piece, (self.ring.owner(way, self.step) * rows, 0)
                )

    def last(self, way=0, number=0):
        return None if self.ring is None else self.held[way][number]

    def whole(self, way, number):
        if self.ring is None:
            return lax.all_gather(self.held[way][number], "row", axis=0, tiled=True)
        return self.built[way][number]


class Scatter:
    def __init__(self, ring, pieces):
        self.ring, self.pieces, self.step = ring, pieces, 0
        if ring is None:
            return
        self.totals = [[self.block(way, part) for part in group] for way, group in enumerate(pieces)]
        self.came = [[None for _ in group] for group in pieces]

    def block(self, way, part):
        rows = part.shape[0] // self.ring.count
        return lax.dynamic_slice_in_dim(part, self.ring.owner(way, self.step + 1) * rows, rows, 0)

    def round(self, *gates, behind=None):
        if self.ring is None:
            return
        self.step += 1
        for way, group in enumerate(self.pieces):
            for number, part in enumerate(group):
                ahead = None if behind is None else behind.last(way, number)
                held = gates if number == len(group) - 1 else ()
                total = after(self.totals[way][number].astype(BF16), ahead, *held)
                came = lax.ppermute(total, "row", self.ring.perms[way])
                self.came[way][number] = came
                own = self.block(way, after(part, came))
                self.totals[way][number] = came.astype(F32) + own.astype(F32)

    def last(self, way=0, number=0):
        return None if self.ring is None else self.came[way][number]

    def result(self, way, number):
        if self.ring is not None:
            return self.totals[way][number]
        return sum_blocks(self.pieces[way][number])


def sum_blocks(part):
    return lax.psum_scatter(part, "row", scatter_dimension=0, tiled=True).astype(F32)


def exchange_sum(ring, values, first):
    if ring is None:
        return lax.psum_scatter(values, "row", scatter_dimension=0, tiled=True)
    bit = ring.count // 2
    rounds = 0
    while bit:
        high = (ring.me & bit) != 0
        half = values.shape[0] // 2
        away = jnp.where(high, values[:half], values[half:])
        came = lax.ppermute(away, "row", [(index, index ^ bit) for index in range(ring.count)])
        values = jnp.where(high, values[half:], values[:half]) + came
        bit //= 2
        if rounds < 2:
            first.round()
            values = after(values, first.last())
            rounds += 1
    return values


def spread_all(ring, values, sums):
    if ring is None:
        return lax.all_gather(values, "row", axis=0, tiled=True)
    bit = 1
    while bit < ring.count:
        high = (ring.me & bit) != 0
        values = after(values, sums.last(0, 0 if bit < 4 else 1))
        came = lax.ppermute(values, "row", [(index, index ^ bit) for index in range(ring.count)])
        values = jnp.concatenate([jnp.where(high, came, values), jnp.where(high, values, came)], axis=0)
        if bit == 1:
            sums.round()
        bit *= 2
    return values


def swaps(bit):
    return [(index, index ^ bit) for index in range(4)]


def gather_features(values):
    if lax.axis_size("col") != 4:
        return lax.all_gather(values, "col", axis=1, tiled=True)
    me = lax.axis_index("col")
    odd, high = (me & 1) == 1, (me & 2) == 2
    far = lax.ppermute(values, "col", swaps(2))
    near = lax.ppermute(values, "col", swaps(1))
    diagonal = lax.ppermute(far, "col", swaps(1))
    mine = [jnp.where(odd, near, values), jnp.where(odd, values, near)]
    other = [jnp.where(odd, diagonal, far), jnp.where(odd, far, diagonal)]
    return jnp.concatenate(
        [jnp.where(high, other[0], mine[0]), jnp.where(high, other[1], mine[1])]
        + [jnp.where(high, mine[0], other[0]), jnp.where(high, mine[1], other[1])],
        axis=1,
    )


def scatter_features(values):
    if lax.axis_size("col") != 4:
        return lax.psum_scatter(values, "col", scatter_dimension=1, tiled=True), None, None
    me = lax.axis_index("col")
    odd, high = (me & 1) == 1, (me & 2) == 2
    width = values.shape[1] // 4
    blocks = [values[:, index * width : (index + 1) * width] for index in range(4)]
    away = jnp.concatenate([jnp.where(odd, blocks[0], blocks[1]), jnp.where(odd, blocks[2], blocks[3])], axis=1)
    step = (away.shape[0] // 4 + 15) // 8 * 8
    cuts = [min(index * step, away.shape[0]) for index in range(5)]
    chunks = [lax.ppermute(away[low:high_row], "col", swaps(1)) for low, high_row in zip(cuts, cuts[1:])]
    came = jnp.concatenate(chunks, axis=0)
    low_sum = jnp.where(odd, blocks[1], blocks[0]) + came[:, :width]
    high_sum = jnp.where(odd, blocks[3], blocks[2]) + came[:, width:]
    last = lax.ppermute(jnp.where(high, low_sum, high_sum).astype(BF16), "col", swaps(2))
    return jnp.where(high, high_sum, low_sum) + last.astype(F32), chunks[-1], last


def slot_table(lengths, image_rows, text_rows):
    slots = lengths.shape[0]
    tables = []
    segments = []
    for column, amount in ((0, image_rows), (1, text_rows)):
        places = jnp.arange(amount, dtype=jnp.int32)[:, None]
        low = jnp.zeros((), jnp.int32)
        segment = jnp.full((amount, 1), slots, jnp.int32)
        for slot in range(slots):
            high = low + lengths[slot, column]
            inside = (places >= low) & (places < high)
            tables.append(inside.astype(F32))
            segment = jnp.where(inside, slot, segment)
            low = high
        segments.append(segment)
    pairs = [jnp.concatenate([tables[slot], tables[slots + slot]], axis=0) for slot in range(slots)]
    return pairs, jnp.concatenate(segments, axis=0)


def stream_dot(left, right_image, right_text):
    upper = jnp.dot(left[:IMG_DEV], right_image, preferred_element_type=F32)
    lower = jnp.dot(left[IMG_DEV:], right_text, preferred_element_type=F32)
    return jnp.concatenate([upper, lower], axis=0)


def stream_dot_back(left, right_image, right_text):
    return stream_dot(left, right_image.T, right_text.T)


def row_mod(members, mod_mine, component):
    streams = []
    for stream, (low, high) in enumerate(((0, IMG_DEV), (IMG_DEV, ROWS))):
        total = None
        for slot, member in enumerate(members):
            term = member[low:high] * mod_mine[slot, 0, stream, component][None, :]
            total = term if total is None else total + term
        streams.append(total)
    return jnp.concatenate(streams, axis=0)


def slot_sums(slot_ones, rows):
    upper = jnp.dot(slot_ones[:IMG_DEV].T, rows[:IMG_DEV], precision=HIGHEST)
    lower = jnp.dot(slot_ones[IMG_DEV:].T, rows[IMG_DEV:], precision=HIGHEST)
    return jnp.stack([upper, lower], axis=1)


def col_sum(values):
    if lax.axis_size("col") != 4:
        return lax.psum(values, "col")
    values = values + lax.ppermute(values, "col", swaps(1))
    return values + lax.ppermute(values, "col", swaps(2))


def feature_sums(first, second, *gates):
    sums = jnp.stack([jnp.sum(first, axis=1), jnp.sum(second, axis=1)], axis=0)
    sums = col_sum(after(sums, *gates))
    return sums[0], sums[1]


def normalize(hidden, *gates):
    totals, squares = feature_sums(hidden, hidden * hidden, *gates)
    center = totals / D
    spread = squares / D - center * center
    scaling = lax.rsqrt(spread + EPSILON)
    return ((hidden - center[:, None]) * scaling[:, None], scaling[:, None])


def norm_back(grad_hat, normed, scaling):
    first, second = feature_sums(grad_hat, grad_hat * normed)
    return scaling * (grad_hat - first[:, None] / D - normed * (second[:, None] / D))


def gelu_slope(value):
    coeff = math.sqrt(2.0 / math.pi)
    tangent = jnp.tanh(coeff * (value + 0.044715 * value * value * value))
    return 0.5 * (1.0 + tangent) + 0.5 * value * (1.0 - tangent * tangent) * coeff * (
        1.0 + 3.0 * 0.044715 * value * value
    )


def silu_slope(value):
    sigma = jax.nn.sigmoid(value)
    return sigma * (1.0 + value * (1.0 - sigma))


def across(left, right):
    return lax.dot_general(left, right, (((1,), (1,)), ((), ())), preferred_element_type=F32)


def down(left, right):
    return lax.dot_general(left, right, (((0,), (0,)), ((), ())), preferred_element_type=F32)


def attend_kernel(q_ref, k_ref, v_ref, seg_keys, seg_queries, out_ref, lse_ref):
    allowed = seg_keys[...] == seg_queries[...]
    for half in range(2):
        lanes = slice(half * HD, (half + 1) * HD)
        queries, key_rows, value_rows = q_ref[:, lanes], k_ref[:, lanes], v_ref[:, lanes]
        scores = jnp.where(allowed, across(key_rows, queries) * (1.0 / math.sqrt(HD)), -jnp.inf)
        highest = jnp.max(scores, axis=0, keepdims=True)
        powers = jnp.exp(scores - highest)
        total = jnp.sum(powers, axis=0, keepdims=True)
        weights = (powers * (1.0 / total)).astype(BF16)
        out_ref[:, lanes] = down(value_rows, weights).T.astype(BF16)
        lse_ref[0, half : half + 1, :] = highest + jnp.log(total)


def attend(queries_keys, value_rows, segments):
    rows, width = value_rows.shape
    pairs = width // (2 * HD)
    block = (rows, 2 * HD)
    return pl.pallas_call(
        attend_kernel,
        grid=(pairs,),
        in_specs=[
            pl.BlockSpec(block, lambda i: (0, i)),
            pl.BlockSpec(block, lambda i: (0, pairs + i)),
            pl.BlockSpec(block, lambda i: (0, i)),
            pl.BlockSpec((rows, 1), lambda i: (0, 0)),
            pl.BlockSpec((1, rows), lambda i: (0, 0)),
        ],
        out_specs=[
            pl.BlockSpec(block, lambda i: (0, i)),
            pl.BlockSpec((1, 8, rows), lambda i: (i, 0, 0)),
        ],
        out_shape=[
            jax.ShapeDtypeStruct((rows, width), BF16),
            jax.ShapeDtypeStruct((pairs, 8, rows), F32),
        ],
        cost_estimate=pl.CostEstimate(
            flops=20 * rows * rows * width, bytes_accessed=10 * rows * width, transcendentals=6 * rows * rows
        ),
        name="attend",
    )(queries_keys, queries_keys, value_rows, segments, segments.reshape(1, rows))


def attend_back_kernel(
    q_ref, k_ref, v_ref, out_ref, grad_ref, lse_ref, seg_keys, seg_queries, dq_ref, dk_ref, dv_ref
):
    allowed = seg_keys[...] == seg_queries[...]
    scale = 1.0 / math.sqrt(HD)
    for half in range(2):
        lanes = slice(half * HD, (half + 1) * HD)
        queries, key_rows, value_rows = q_ref[:, lanes], k_ref[:, lanes], v_ref[:, lanes]
        grads = grad_ref[:, lanes]
        products = grads.astype(F32) * out_ref[:, lanes].astype(F32)
        inner = jnp.sum(products.T, axis=0, keepdims=True)
        scores = across(key_rows, queries) * scale
        probs = jnp.where(allowed, jnp.exp(scores - lse_ref[0, half : half + 1, :]), 0.0)
        dv_ref[:, lanes] = jnp.dot(probs.astype(BF16), grads, preferred_element_type=F32).astype(BF16)
        grad_probs = across(value_rows, grads)
        grad_scores = (probs * (grad_probs - inner) * scale).astype(BF16)
        dk_ref[:, lanes] = jnp.dot(grad_scores, queries, preferred_element_type=F32).astype(BF16)
        dq_ref[:, lanes] = down(key_rows, grad_scores).T.astype(BF16)


def attend_back(queries_keys, value_rows, attended, grads, log_totals, segments):
    rows, width = value_rows.shape
    pairs = width // (2 * HD)
    block = (rows, 2 * HD)
    plain = pl.BlockSpec(block, lambda i: (0, i))
    return pl.pallas_call(
        attend_back_kernel,
        grid=(pairs,),
        in_specs=[
            plain,
            pl.BlockSpec(block, lambda i: (0, pairs + i)),
            plain,
            plain,
            plain,
            pl.BlockSpec((1, 8, rows), lambda i: (i, 0, 0)),
            pl.BlockSpec((rows, 1), lambda i: (0, 0)),
            pl.BlockSpec((1, rows), lambda i: (0, 0)),
        ],
        out_specs=[plain] * 3,
        out_shape=[jax.ShapeDtypeStruct((rows, width), BF16)] * 3,
        cost_estimate=pl.CostEstimate(
            flops=40 * rows * rows * width, bytes_accessed=20 * rows * width, transcendentals=6 * rows * rows
        ),
        name="attend_back",
    )(
        queries_keys,
        queries_keys,
        value_rows,
        attended,
        grads,
        log_totals,
        segments,
        segments.reshape(1, rows),
    )


def part_of(left, right, low, high):
    return jnp.einsum("nk,nf->kf", left[low:high], right[low:high], preferred_element_type=F32).astype(BF16)


STREAMS = ((0, IMG_DEV), (IMG_DEV, ROWS))


def per_device(
    image_in,
    text_in,
    condition,
    ranges,
    mod_weight,
    qkv_weight,
    out_weight,
    up_weight,
    down_weight,
    image_cot,
    text_cot,
):
    members, segments = slot_table(ranges, IMG_DEV, TXT_DEV)
    slot_ones = jnp.concatenate(members, axis=1)
    col_width = image_in.shape[1]
    ff_width = up_weight.shape[3]
    half_ff = ff_width // 2
    size = lax.axis_size("row")
    ring = Ring(size) if size <= RING_LIMIT else None

    qkv_local, out_local = qkv_weight[0], out_weight[0]
    up_local, down_local = up_weight[0], down_weight[0]
    first_pieces = [
        [
            jnp.concatenate([qkv_local[:, way, 0], qkv_local[:, way, 1]], axis=1),
            jnp.concatenate([qkv_local[:, way, 2], out_local[:, way]], axis=1),
        ]
        for way in range(2)
    ]
    halves = lambda weight: [[weight[:, way, :half_ff], weight[:, way, half_ff:]] for way in range(2)]
    first, up, last = (
        Gather(ring, first_pieces),
        Gather(ring, halves(up_local)),
        Gather(ring, halves(down_local)),
    )

    def part_dot(left, source, part):
        return stream_dot(left, source.whole(0, part), source.whole(1, part))

    def part_back(left, source, part):
        return stream_dot_back(left, source.whole(0, part), source.whole(1, part))

    silu_cond = jax.nn.silu(condition.astype(F32)).astype(BF16)
    mod_terms = jnp.einsum("sd,ldxkf->slxkf", silu_cond, mod_weight, preferred_element_type=F32)
    first.round()
    mod_mine = exchange_sum(ring, mod_terms, first)
    hidden = jnp.concatenate([image_in, text_in], axis=0).astype(F32)
    normed_one, scaling_one = normalize(hidden, first.last())
    mods = [row_mod(members, mod_mine, part_no) for part_no in range(6)]
    modulated_one = (normed_one * (1.0 + mods[1]) + mods[0]).astype(BF16)
    gathered_one = gather_features(modulated_one)
    while first.step < 3:
        first.round()
    grad_hidden = jnp.concatenate([image_cot, text_cot], axis=0).astype(F32)
    grad_branch_two = (grad_hidden * mods[5]).astype(BF16)
    first.round()
    first.round(modulated_one)
    first.round(gathered_one)
    first.round()
    up.round(behind=first)

    qk_whole = [first.whole(way, 0) for way in range(2)]
    v_whole = [first.whole(way, 1)[:, :col_width] for way in range(2)]
    out_whole = [first.whole(way, 1)[:, col_width:] for way in range(2)]
    queries_keys = stream_dot(gathered_one, *qk_whole).astype(BF16)
    value_rows = stream_dot(after(gathered_one, up.last()), *v_whole).astype(BF16)
    up.round()
    mixed, log_totals = attend(queries_keys, after(value_rows, up.last()), segments)
    up.round()
    branch_one, stage, stage_two = scatter_features(stream_dot_back(mixed, *out_whole))
    grad_full_two = gather_features(after(grad_branch_two, up.last()))
    up.round(mixed)
    up.round(stage)
    midway = hidden + mods[2] * branch_one
    normed_two, scaling_two = normalize(midway)
    modulated_two = (normed_two * (1.0 + mods[4]) + mods[3]).astype(BF16)
    up.round(stage_two)
    up.round(modulated_two)
    gathered_two = gather_features(modulated_two)
    last.round(behind=up)
    last.round()
    lifted, activated, down_parts = [], [], [[], []]
    for part in range(2):
        lifted.append(part_dot(after(gathered_two, last.last()), up, part))
        activated.append(jax.nn.gelu(lifted[part], approximate=True).astype(BF16))
        last.round(activated[part] if part else gathered_two)
    for part in range(2):
        given = after(grad_full_two, last.last())
        for way, (low, high) in enumerate(STREAMS):
            down_parts[way].append(part_of(given, activated[part], low, high))
        last.round(down_parts[1][part])
    last.round()

    down_sums = Scatter(ring, down_parts)
    down_sums.round(behind=last)
    grad_lifted = []
    for part in range(2):
        grad_act = part_dot(after(grad_full_two, down_sums.last()), last, part)
        grad_lifted.append((grad_act * gelu_slope(lifted[part])).astype(BF16))
        down_sums.round(grad_lifted[part] if part else None)
    lower_part = part_back(after(grad_lifted[0], down_sums.last()), up, 0)
    down_sums.round()
    grad_mod_two, stage, stage_two = scatter_features(
        lower_part + part_back(after(grad_lifted[1], down_sums.last()), up, 1)
    )
    down_sums.round()
    up_parts = [[], []]
    for part in range(2):
        given = after(gathered_two, down_sums.last())
        for way, (low, high) in enumerate(STREAMS):
            up_parts[way].append(part_of(given, grad_lifted[part], low, high))
        down_sums.round(up_parts[1][part], stage)
    up_sums = Scatter(ring, up_parts)
    up_sums.round(stage_two, behind=down_sums)
    scale_two_rows = grad_mod_two * normed_two
    grad_hidden_two = grad_hidden
    grad_hidden = grad_hidden + norm_back(grad_mod_two * (1.0 + mods[4]), normed_two, scaling_two)
    grad_branch_one = (grad_hidden * mods[2]).astype(BF16)
    gate_one_rows = grad_hidden * branch_one
    lower_part = part_back(after(activated[0], up_sums.last()), last, 0)
    up_sums.round(grad_branch_one)
    grad_full_one = gather_features(grad_branch_one)
    branch_two, _, stage_far = scatter_features(
        lower_part + part_back(after(activated[1], up_sums.last()), last, 1)
    )
    branch_two = after(branch_two, grad_full_one)
    hidden = midway + mods[5] * branch_two
    image_out = hidden[:IMG_DEV]
    text_out = hidden[IMG_DEV:]
    gate_two_rows = grad_hidden_two * branch_two
    up_sums.round()
    grad_mixed = stream_dot(after(grad_full_one, up_sums.last()), *out_whole).astype(BF16)
    up_sums.round(grad_mixed)
    grad_q, grad_k, grad_v = attend_back(
        queries_keys, value_rows, mixed, after(grad_mixed, up_sums.last()), log_totals, segments
    )
    grad_qk = jnp.concatenate([grad_q, grad_k], axis=1)
    up_sums.round()
    qk_parts = [part_of(gathered_one, after(grad_qk, up_sums.last()), low, high) for low, high in STREAMS]
    up_sums.round(grad_v, stage_far)
    given = after(gathered_one, up_sums.last())
    other_parts = [
        jnp.concatenate([part_of(given, grad_v, low, high), part_of(grad_full_one, mixed, low, high)], axis=1)
        for low, high in STREAMS
    ]
    up_sums.round(qk_parts[1])
    first_sums = Scatter(ring, [[qk_parts[way], other_parts[way]] for way in range(2)])
    first_sums.round(behind=up_sums)
    grad_mod_one, stage, stage_two = scatter_features(
        stream_dot_back(after(grad_qk, first_sums.last()), *qk_whole) + stream_dot_back(grad_v, *v_whole)
    )
    first_sums.round()
    first_sums.round(stage)
    scale_one_rows = grad_mod_one * normed_one
    grad_hidden = grad_hidden + norm_back(grad_mod_one * (1.0 + mods[1]), normed_one, scaling_one)
    rows_list = [
        grad_mod_one,
        scale_one_rows,
        gate_one_rows,
        grad_mod_two,
        scale_two_rows,
        gate_two_rows,
    ]
    slot_grads = jnp.stack([slot_sums(slot_ones, rows) for rows in rows_list], axis=2)
    first_sums.round(stage_two)
    mod_all = spread_all(ring, slot_grads[:, None], first_sums)
    grad_mod = jnp.einsum("sd,slxkf->ldxkf", silu_cond.astype(F32), mod_all, precision=HIGHEST)
    cond_part = jnp.einsum("slxkf,ldxkf->sd", mod_all, mod_weight.astype(F32), precision=HIGHEST)
    cond_total = col_sum(cond_part)
    grad_cond = cond_total * silu_slope(condition.astype(F32))
    while ring is not None and first_sums.step < size - 1:
        first_sums.round(mod_all if first_sums.step == size - 2 else None)
    gather_sums = lambda sums: [[sums.result(way, number) for number in range(2)] for way in range(2)]
    grads_first, grads_up, grads_down = (gather_sums(sums) for sums in (first_sums, up_sums, down_sums))

    def stacked(grads):
        return jnp.stack([jnp.concatenate(parts, axis=1) for parts in grads], axis=1)

    grad_qkv = jnp.stack(
        [
            jnp.stack(
                [parts[0][:, :col_width], parts[0][:, col_width:], parts[1][:, :col_width]],
                axis=1,
            )
            for parts in grads_first
        ],
        axis=1,
    )
    grad_out = jnp.stack([parts[1][:, col_width:] for parts in grads_first], axis=1)
    return (
        image_out,
        text_out,
        grad_hidden[:IMG_DEV],
        grad_hidden[IMG_DEV:],
        grad_cond,
        grad_mod,
        grad_qkv[None],
        grad_out[None],
        stacked(grads_up)[None],
        stacked(grads_down)[None],
    )


def solution(mesh):
    return jax.shard_map(
        per_device,
        mesh=mesh,
        in_specs=(
            P("row", "col"),
            P("row", "col"),
            P(None, "row"),
            P("row", None),
            P(None, "row", None, None, "col"),
            P(None, "row", None, None, "col"),
            P(None, "row", None, "col"),
            P(None, "row", None, "col"),
            P(None, "row", None, "col"),
            P("row", "col"),
            P("row", "col"),
        ),
        out_specs=(
            P("row", "col"),
            P("row", "col"),
            P("row", "col"),
            P("row", "col"),
            P(None, "row"),
            P(None, "row", None, None, "col"),
            P(None, "row", None, None, "col"),
            P(None, "row", None, "col"),
            P(None, "row", None, "col"),
            P(None, "row", None, "col"),
        ),
        check_vma=False,
    )
```
